32 devices in a mesh: row: 8 (over z, x), col: 2 (over core), dp: 2 (over y).
Axes of the slice: x: 2, y: 2, z: 4, core: 2. Of those that a mesh axis runs over, the one named last changes fastest.
Arguments:
- pixels: bfloat16 [2, 3, 256, 256], P('dp', None, 'row', 'col'), may hold values from -6 to 6
- cotangent: bfloat16 [2, 64, 64, 1024], P('dp', 'row', 'col'), may hold values from -6 to 6
- embed_weight: bfloat16 [48, 1024], replicated, may hold values from -0.875 to 0.875
- embed_bias: float32 [1024], replicated, may hold values from -4 to 4
- layer_norm_gain: float32 [1024], replicated, may hold values from 0.5 to 1.5
- qkv_weight: bfloat16 [1024, 2304], P('row', ('col', 'dp')), may hold values from -0.1875 to 0.1875
- out_weight: bfloat16 [768, 1024], P('row', ('col', 'dp')), may hold values from -0.21875 to 0.21875
- bias_table: float32 [12, 225], replicated, may hold values from -4 to 404
- rel_index: int32 [64, 64], replicated, may hold values from 0 to 224
- shifts: int32 [2, 2], P('dp'), may hold values from 1 to 7
Outputs:
- out_weight_grad: float32 [768, 1024], P('row', ('col', 'dp'))
- embed_weight_grad: float32 [48, 1024], replicated
- embed_bias_grad: float32 [1024], replicated
- norm_gain_grad: float32 [1024], replicated
- bias_table_grad: float32 [12, 225], replicated
The draws below stay inside these ranges and needn't reach their ends.
Inputs may be any that keep to these rules, and one draw needn't show every extreme that they name: `rel_index`: each entry names one of the 225 columns of bias_table.
All inputs are finite; a program needn't handle non-finite values.
Results may differ from the reference program's by a relative error of at most 0.023.
Values may be sent and summed in bfloat16 or wider, within the bound.
A program may use at most 64 MiB of HBM per device.

```python
import jax
import jax.numpy as jnp
from jax import lax

D = 1024
HEADS = 12
WIN = 8
PATCH = 4
CHAN = 3
HD = 768
TABLE = 225
KDIM = 48
BATCH = 2
GRID_ROWS = 64
GRID_COLS = 64
PIX_ROWS = 256
PIX_COLS = 256


def draw_bias_table(key, part):
    key_base = jax.random.fold_in(key, 11)
    base_draw = jax.random.normal(key_base, (HEADS, TABLE), jnp.float32)
    return jnp.clip(base_draw, -4.0, 4.0)


def with_ends(entries, own_key, smallest, top_value):
    place = [jax.random.randint(jax.random.fold_in(own_key, axis), (), 0, length) for axis, length in enumerate(entries.shape)]
    longest = entries.shape.index(max(entries.shape))
    next_to = place[:longest] + [(place[longest] + 1) % entries.shape[longest]] + place[longest + 1:]
    return entries.at[tuple(place)].set(smallest).at[tuple(next_to)].set(top_value)


def block_levels(key, extent, shards, least, largest):
    factor_of = 1.0
    for dim, shards_of in shards:
        draws = jax.random.uniform(jax.random.fold_in(jax.random.fold_in(key, 6), dim), (shards_of,), jnp.float32, least / len(shards), largest / len(shards))
        factor_of = factor_of * jnp.repeat(jnp.exp(draws), extent[dim] // shards_of).reshape((-1,) + (1,) * (len(extent) - 1 - dim))
    return factor_of


def gaussian(own_key, dims, spread, most, pieces=(), kind=jnp.bfloat16):
    entries = spread * jax.random.normal(own_key, dims, jnp.float32)
    if pieces:
        entries = entries * block_levels(own_key, dims, pieces, -0.22, 0.18)
    return jnp.clip(entries, -most, most).astype(kind)


def setup_inputs(seed: int = 0) -> dict:
    splits = jax.random.split(jax.random.key(seed), 11)
    return {
        "pixels": gaussian(splits[0], (BATCH, CHAN, PIX_ROWS, PIX_COLS), 1.0, 6.0, ((0, 2), (2, 8), (3, 2))),
        "cotangent": gaussian(splits[1], (BATCH, GRID_ROWS, GRID_COLS, D), 1.0, 6.0, ((0, 2), (1, 8), (2, 2))),
        "embed_weight": gaussian(splits[2], (KDIM, D), KDIM ** -0.5, 0.875),
        "embed_bias": gaussian(splits[3], (D,), 1.0, 4.0, (), jnp.float32),
        "layer_norm_gain": jnp.clip(1.0 + 0.1 * jax.random.normal(splits[4], (D,), jnp.float32), 0.5, 1.5),
        "qkv_weight": gaussian(splits[5], (D, 3 * HD), D ** -0.5, 0.1875, ((0, 8), (1, 4))),
        "out_weight": gaussian(splits[6], (HD, D), HD ** -0.5, 0.21875, ((0, 8), (1, 4))),
        "bias_table": draw_bias_table(jax.random.fold_in(splits[10], 71), 0),
        "rel_index": with_ends(jax.random.randint(splits[8], (WIN * WIN, WIN * WIN), 0, TABLE), jax.random.fold_in(splits[8], 1), 0, TABLE - 1).astype(jnp.int32),
        "shifts": with_ends(jax.random.randint(splits[9], (BATCH, 2), 1, WIN), jax.random.fold_in(splits[9], 1), 1, WIN - 1).astype(jnp.int32),
    }


norm_epsilon = 1e-05

def make_patches(pixel_block):
    images, channels, pixel_rows, pixel_cols = pixel_block.shape
    grid_rows = pixel_rows // PATCH
    grid_cols = pixel_cols // PATCH
    shaped = pixel_block.reshape(images, channels, grid_rows, PATCH, grid_cols, PATCH)
    return shaped.transpose(0, 2, 4, 1, 3, 5).reshape(images, grid_rows, grid_cols, channels * PATCH * PATCH)

def window_split(block):
    rows_all, cols_all, features = block.shape
    shaped = block.reshape(rows_all // WIN, WIN, cols_all // WIN, WIN, features)
    return shaped.transpose(0, 2, 1, 3, 4).reshape(-1, WIN * WIN, features)

def window_join(windows, rows_all, cols_all):
    features = windows.shape[-1]
    shaped = windows.reshape(rows_all // WIN, cols_all // WIN, WIN, WIN, features)
    return shaped.transpose(0, 2, 1, 3, 4).reshape(rows_all, cols_all, features)

def window_grads(cell_windows, cot_windows, labels, layer_norm_gain, qkv_weight, out_weight, bias_full):
    window_count, cell_count, features = cell_windows.shape
    head_count = bias_full.shape[0]
    inner_width = out_weight.shape[0]
    head_size = inner_width // head_count
    score_scale = head_size ** (-0.5)
    flat_rows = cell_windows.reshape(-1, features).astype(jnp.float32)
    average = lax.optimization_barrier(jnp.mean(flat_rows, axis=-1, keepdims=True))
    centered_input = flat_rows - average
    inverse_deviation = lax.rsqrt(lax.optimization_barrier(jnp.mean(centered_input * centered_input, axis=-1, keepdims=True)) + norm_epsilon)
    standardized_rows = centered_input * inverse_deviation
    normalized_rows = (standardized_rows * layer_norm_gain).astype(jnp.bfloat16)
    projected = jnp.dot(normalized_rows, qkv_weight, preferred_element_type=jnp.float32).astype(jnp.bfloat16)
    head_shape = (window_count, cell_count, head_count, head_size)
    query_rows = projected[:, :inner_width].reshape(head_shape).astype(jnp.float32)
    key_vectors = projected[:, inner_width:2 * inner_width].reshape(head_shape).astype(jnp.float32)
    value_rows = projected[:, 2 * inner_width:].reshape(head_shape).astype(jnp.float32)
    scores = jnp.einsum('wmhd,wnhd->whmn', query_rows, key_vectors) * score_scale + bias_full[None]
    same_region = labels[:, None, :, None] == labels[:, None, None, :]
    scores = jnp.where(same_region, scores, -1e+30)
    row_peak = lax.optimization_barrier(jnp.max(scores, axis=-1, keepdims=True))
    exp_scores = jnp.exp(scores - row_peak)
    attention_weights = exp_scores / lax.optimization_barrier(jnp.sum(exp_scores, axis=-1, keepdims=True))
    reduced_probability = attention_weights.astype(jnp.bfloat16)
    attended = jnp.einsum('whmn,wnhd->wmhd', reduced_probability.astype(jnp.float32), value_rows).astype(jnp.bfloat16)
    cot_rows = cot_windows.reshape(-1, features)
    d_attended = jnp.dot(cot_rows, out_weight.T, preferred_element_type=jnp.float32).astype(jnp.bfloat16)
    d_heads = d_attended.reshape(head_shape).astype(jnp.float32)
    d_prob = jnp.einsum('wmhd,wnhd->whmn', d_heads, value_rows)
    d_values = jnp.einsum('whmn,wmhd->wnhd', reduced_probability.astype(jnp.float32), d_heads).astype(jnp.bfloat16)
    d_scores = attention_weights * (d_prob - lax.optimization_barrier(jnp.sum(attention_weights * d_prob, axis=-1, keepdims=True)))
    table_part = lax.optimization_barrier(jnp.sum(d_scores, axis=0))
    d_low = d_scores.astype(jnp.bfloat16).astype(jnp.float32)
    d_queries = (jnp.einsum('whmn,wnhd->wmhd', d_low, key_vectors) * score_scale).astype(jnp.bfloat16)
    d_keys = (jnp.einsum('whmn,wmhd->wnhd', d_low, query_rows) * score_scale).astype(jnp.bfloat16)
    total_row_count = flat_rows.shape[0]
    d_projected = jnp.concatenate([d_queries.reshape(total_row_count, inner_width), d_keys.reshape(total_row_count, inner_width), d_values.reshape(total_row_count, inner_width)], axis=1)
    normalized_gradient = jnp.dot(d_projected, qkv_weight.T, preferred_element_type=jnp.float32)
    gain_contribution = lax.optimization_barrier(jnp.sum(normalized_gradient * standardized_rows, axis=0))
    scaled_rows = normalized_gradient * layer_norm_gain
    branch_gradient = inverse_deviation * (scaled_rows - lax.optimization_barrier(jnp.mean(scaled_rows, axis=-1, keepdims=True)) - standardized_rows * lax.optimization_barrier(jnp.mean(scaled_rows * standardized_rows, axis=-1, keepdims=True)))
    attended_rows = attended.reshape(total_row_count, inner_width)
    return (branch_gradient.astype(jnp.bfloat16), attended_rows, gain_contribution, table_part)

def reference(pixels, cotangent, embed_weight, embed_bias, layer_norm_gain, qkv_weight, out_weight, bias_table, rel_index, shifts):
    images, grid_rows, grid_cols, features = cotangent.shape
    head_count = bias_table.shape[0]
    table_size = bias_table.shape[1]
    inner_width = out_weight.shape[0]
    patch_width = embed_weight.shape[0]
    selector = (rel_index.reshape(-1)[:, None] == jnp.arange(table_size, dtype=jnp.int32)[None, :]).astype(jnp.float32)
    bias_full = jnp.dot(selector, bias_table.T, precision=lax.Precision.HIGHEST).T.reshape(head_count, WIN * WIN, WIN * WIN)
    patches_all = make_patches(pixels)
    band_count = grid_rows // WIN

    def per_image(carry, inputs):
        out_grad, embed_grad, bias_grad, gain_grad, table_grad = carry
        patches, cot_image, shift_pair = inputs
        tokens = (jnp.dot(patches, embed_weight, preferred_element_type=jnp.float32) + embed_bias).astype(jnp.bfloat16)
        shifted = jnp.roll(jnp.roll(tokens, -shift_pair[0], axis=0), -shift_pair[1], axis=1)
        shifted_cot = jnp.roll(jnp.roll(cot_image, -shift_pair[0], axis=0), -shift_pair[1], axis=1)
        band_tokens = shifted.reshape(band_count, WIN, grid_cols, features)
        band_cots = shifted_cot.reshape(band_count, WIN, grid_cols, features)

        def per_band(inner, band_inputs):
            band_out, band_gain, band_table = inner
            band_x, band_c, band_index = band_inputs
            row_ids = band_index * WIN + jnp.arange(WIN, dtype=jnp.int32)
            col_ids = jnp.arange(grid_cols, dtype=jnp.int32)
            row_part = (row_ids[:, None] >= grid_rows - shift_pair[0]).astype(jnp.int32)
            col_part = (col_ids[None, :] >= grid_cols - shift_pair[1]).astype(jnp.int32)
            region = 2 * row_part + col_part
            labels = window_split(region[:, :, None])[:, :, 0]
            cell_windows = window_split(band_x)
            cot_windows = window_split(band_c)
            branch_gradient, attended_rows, gain_contribution, table_part = window_grads(cell_windows, cot_windows, labels, layer_norm_gain, qkv_weight, out_weight, bias_full)
            band_out = band_out + lax.dot_general(attended_rows, cot_windows.reshape(-1, features), (((0,), (0,)), ((), ())), preferred_element_type=jnp.float32)
            joined = window_join(branch_gradient.reshape(-1, WIN * WIN, features), WIN, grid_cols)
            return ((band_out, band_gain + gain_contribution, band_table + table_part), joined)
        band_ids = jnp.arange(band_count, dtype=jnp.int32)
        (out_grad, gain_grad, table_grad), d_bands = lax.scan(per_band, (out_grad, gain_grad, table_grad), (band_tokens, band_cots, band_ids))
        branch_gradient = d_bands.reshape(grid_rows, grid_cols, features)
        d_back = jnp.roll(jnp.roll(branch_gradient, shift_pair[0], axis=0), shift_pair[1], axis=1)
        patch_rows = patches.reshape(-1, patch_width)
        cot_rows = cot_image.reshape(-1, features)
        back_rows = d_back.reshape(-1, features)
        contract = (((0,), (0,)), ((), ()))
        embed_grad = embed_grad + lax.dot_general(patch_rows, cot_rows, contract, preferred_element_type=jnp.float32) + lax.dot_general(patch_rows, back_rows, contract, preferred_element_type=jnp.float32)
        bias_grad = bias_grad + lax.optimization_barrier(jnp.sum(cot_rows, axis=0, dtype=jnp.float32)) + lax.optimization_barrier(jnp.sum(back_rows, axis=0, dtype=jnp.float32))
        return ((out_grad, embed_grad, bias_grad, gain_grad, table_grad), None)
    initial = (jnp.zeros((inner_width, features), jnp.float32), jnp.zeros((patch_width, features), jnp.float32), jnp.zeros((features,), jnp.float32), jnp.zeros((features,), jnp.float32), jnp.zeros((head_count, WIN * WIN, WIN * WIN), jnp.float32))
    totals, unused = lax.scan(per_image, initial, (patches_all, cotangent, shifts))
    out_grad, embed_grad, bias_grad, gain_grad, table_grad = totals
    table_result = jnp.dot(table_grad.reshape(head_count, -1), selector, precision=lax.Precision.HIGHEST)
    return (out_grad, embed_grad, bias_grad, gain_grad, table_result)
```

```python
import functools

import jax
import jax.numpy as jnp
from jax import lax
from jax.experimental import pallas as pl
from jax.experimental.pallas import tpu as pltpu
from jax.sharding import PartitionSpec as P

WIN = 8
PATCH = 4


norm_epsilon = 1e-05


def from_behind(value, axis, steps):
    count = lax.axis_size(axis)
    pairs = [(source, (source + steps) % count) for source in range(count)]
    return lax.ppermute(value, axis, pairs)


def make_patches(pixel_block):
    images, channels, pixel_rows, pixel_cols = pixel_block.shape
    grid_rows = pixel_rows // PATCH
    grid_cols = pixel_cols // PATCH
    shaped = pixel_block.reshape(images, channels, grid_rows, PATCH, grid_cols, PATCH)
    return shaped.transpose(0, 2, 4, 1, 3, 5).reshape(
        images, grid_rows, grid_cols, channels * PATCH * PATCH
    )


def embed_cells(patches, embed_weight, embed_bias):
    return (jnp.dot(patches, embed_weight, preferred_element_type=jnp.float32) + embed_bias).astype(
        jnp.bfloat16
    )


def window_split(block):
    rows_all, cols_all, features = block.shape
    shaped = block.reshape(rows_all // WIN, WIN, cols_all // WIN, WIN, features)
    return shaped.transpose(0, 2, 1, 3, 4).reshape(-1, WIN * WIN, features)


def window_join(windows, rows_all, cols_all):
    features = windows.shape[-1]
    shaped = windows.reshape(rows_all // WIN, cols_all // WIN, WIN, WIN, features)
    return shaped.transpose(0, 2, 1, 3, 4).reshape(rows_all, cols_all, features)

def attend_forward(cell_windows, labels, layer_norm_gain, qkv_full, bias_full):
    window_count, cell_count, features = cell_windows.shape
    head_count = bias_full.shape[0]
    inner_width = qkv_full.shape[1] // 3
    head_size = inner_width // head_count
    score_scale = head_size ** (-0.5)
    flat_rows = cell_windows.reshape(-1, features).astype(jnp.float32)
    average = jnp.mean(flat_rows, axis=-1, keepdims=True)
    centered_input = flat_rows - average
    inverse_deviation = lax.rsqrt(
        jnp.mean(centered_input * centered_input, axis=-1, keepdims=True) + norm_epsilon
    )
    standardized_rows = centered_input * inverse_deviation
    normalized_rows = (standardized_rows * layer_norm_gain).astype(jnp.bfloat16)
    projected = jnp.dot(normalized_rows, qkv_full, preferred_element_type=jnp.float32).astype(
        jnp.bfloat16
    )
    head_shape = (window_count, cell_count, head_count, head_size)
    query_rows = projected[:, :inner_width].reshape(head_shape)
    key_vectors = projected[:, inner_width : 2 * inner_width].reshape(head_shape)
    value_rows = projected[:, 2 * inner_width :].reshape(head_shape)
    scores = (
        jnp.einsum("wmhd,wnhd->whmn", query_rows, key_vectors, preferred_element_type=jnp.float32)
        * score_scale
        + bias_full[None]
    )
    same_region = labels[:, None, :, None] == labels[:, None, None, :]
    scores = jnp.where(same_region, scores, -1e30)
    row_peak = jnp.max(scores, axis=-1, keepdims=True)
    exp_scores = jnp.exp(scores - row_peak)
    attention_weights = exp_scores / jnp.sum(exp_scores, axis=-1, keepdims=True)
    reduced_probability = attention_weights.astype(jnp.bfloat16)
    attended = jnp.einsum(
        "whmn,wnhd->wmhd", reduced_probability, value_rows, preferred_element_type=jnp.float32
    ).astype(jnp.bfloat16)
    stored_residuals = (
        standardized_rows,
        inverse_deviation,
        query_rows,
        key_vectors,
        value_rows,
        attention_weights,
        reduced_probability,
    )
    return (stored_residuals, attended.reshape(-1, inner_width))


def attend_backward(stored_residuals, d_attended, layer_norm_gain, qkv_full):
    (
        standardized_rows,
        inverse_deviation,
        query_rows,
        key_vectors,
        value_rows,
        attention_weights,
        reduced_probability,
    ) = stored_residuals
    head_shape = query_rows.shape
    score_scale = head_shape[3] ** (-0.5)
    total_row_count = standardized_rows.shape[0]
    inner_width = head_shape[2] * head_shape[3]
    d_heads = d_attended.reshape(head_shape)
    d_prob = jnp.einsum("wmhd,wnhd->whmn", d_heads, value_rows, preferred_element_type=jnp.float32)
    d_values = jnp.einsum(
        "whmn,wmhd->wnhd", reduced_probability, d_heads, preferred_element_type=jnp.float32
    ).astype(jnp.bfloat16)
    d_scores = attention_weights * (
        d_prob - jnp.sum(attention_weights * d_prob, axis=-1, keepdims=True)
    )
    table_part = jnp.sum(d_scores, axis=0)
    d_low = d_scores.astype(jnp.bfloat16)
    d_queries = (
        jnp.einsum("whmn,wnhd->wmhd", d_low, key_vectors, preferred_element_type=jnp.float32)
        * score_scale
    ).astype(jnp.bfloat16)
    d_keys = (
        jnp.einsum("whmn,wmhd->wnhd", d_low, query_rows, preferred_element_type=jnp.float32)
        * score_scale
    ).astype(jnp.bfloat16)
    d_projected = jnp.concatenate(
        [
            d_queries.reshape(total_row_count, inner_width),
            d_keys.reshape(total_row_count, inner_width),
            d_values.reshape(total_row_count, inner_width),
        ],
        axis=1,
    )
    normalized_gradient = lax.dot_general(
        d_projected, qkv_full, (((1,), (1,)), ((), ())), preferred_element_type=jnp.float32
    )
    gain_contribution = jnp.sum(normalized_gradient * standardized_rows, axis=0)
    scaled_rows = normalized_gradient * layer_norm_gain
    branch_gradient = inverse_deviation * (
        scaled_rows
        - jnp.mean(scaled_rows, axis=-1, keepdims=True)
        - standardized_rows * jnp.mean(scaled_rows * standardized_rows, axis=-1, keepdims=True)
    )
    return (branch_gradient.astype(jnp.bfloat16), gain_contribution, table_part)


MESH = pl.DeviceIdType.MESH
VMEM = pltpu.VMEM


def greet_everyone(sizes, row, col, dp):
    rows, cols, dps = sizes
    barrier = pltpu.get_barrier_semaphore()
    others = 0
    for r in range(rows):
        for c in range(cols):
            for d in range(dps):
                if r or c or d:
                    others += 1
                    pl.semaphore_signal(
                        barrier,
                        inc=1,
                        device_id={
                            "row": (row + r) % rows,
                            "col": (col + c) % cols,
                            "dp": (dp + d) % dps,
                        },
                        device_id_type=MESH,
                    )
    pl.semaphore_wait(barrier, others)


def gather_kernel(
    sizes, qkv_ref, out_ref, cot_ref, pix_ref,
    qkv_all, out_all, cot_r, cot_c, cot_x, pix_r, pix_c, pix_x,
    send_sem, recv_sem, own_sem, halo_send, halo_recv,
):
    rows, cols, _ = sizes
    ring = rows // 2
    row, col, dp = lax.axis_index("row"), lax.axis_index("col"), lax.axis_index("dp")
    x, z = row % 2, row // 2
    greet_everyone(sizes, row, col, dp)
    gathered = (qkv_all, out_all)
    own = (qkv_ref, out_ref)
    started = []

    def slot(array, ident):
        flag, dy, dx, dz = ident
        column = (col + flag) % 2
        which_row = ((z - dz + ring) % ring) * 2 + (x + dx) % 2
        return gathered[array].at[column * 2 + (dp + dy) % 2, which_row]

    def semaphore(array, ident):
        flag, dy, dx, dz = ident
        return recv_sem.at[array, ((flag * 2 + dy) * 2 + dx) * ring + dz]

    def send(ident, device, landing):
        for array in range(2):
            source = own[array] if ident == (0, 0, 0, 0) else slot(array, ident)
            copy = pltpu.make_async_remote_copy(
                src_ref=source,
                dst_ref=slot(array, ident),
                send_sem=send_sem.at[len(started)],
                recv_sem=semaphore(array, landing),
                device_id=device,
                device_id_type=MESH,
            )
            copy.start()
            started.append(copy)

    def arrive(ident):
        for array in range(2):
            pltpu.make_async_remote_copy(
                src_ref=slot(array, ident),
                dst_ref=slot(array, ident),
                send_sem=send_sem.at[0],
                recv_sem=semaphore(array, ident),
                device_id={"col": (col + 1) % 2},
                device_id_type=MESH,
            ).wait_recv()

    over_y = {"dp": (dp + 1) % 2}
    over_x = {"row": z * 2 + (x + 1) % 2}
    up = {"row": ((z + 1) % ring) * 2 + x}
    down = {"row": ((z + ring - 1) % ring) * 2 + x}
    over_core = {"col": (col + 1) % 2}

    def onward_up(dy, dx, dz):
        if dz + 1 < ring // 2 or (dz + 1 == ring // 2 and dy == 0):
            send((0, dy, dx, dz), up, (0, dy, dx, dz + 1))

    def onward_down(dy, dx, back):
        if back + 1 < ring // 2 or (back + 1 == ring // 2 and dy == 1):
            send((0, dy, dx, (ring - back) % ring), down, (0, dy, dx, ring - back - 1))

    def spread(dy, dx):
        onward_up(dy, dx, 0)
        onward_down(dy, dx, 0)

    send((0, 0, 0, 0), over_y, (0, 1, 0, 0))
    send((0, 0, 0, 0), over_x, (0, 0, 1, 0))
    spread(0, 0)
    send((0, 0, 0, 0), over_core, (1, 0, 0, 0))
    local = [
        pltpu.make_async_copy(own[array], slot(array, (0, 0, 0, 0)), own_sem.at[array])
        for array in range(2)
    ]
    for copy in local:
        copy.start()
    arrive((0, 1, 0, 0))
    send((0, 1, 0, 0), over_x, (0, 1, 1, 0))
    spread(1, 0)
    above = (row + rows - 1) % rows
    left = (col + cols - 1) % cols
    edge = cot_c.shape[1]
    halos = []
    for source, target, device in (
        (pix_ref, pix_r, {"row": above}),
        (pix_ref, pix_c, {"col": left}),
        (pix_ref, pix_x, {"row": above, "col": left}),
        (cot_ref, cot_r, {"row": above}),
        (cot_ref.at[:, pl.ds(0, edge)], cot_c, {"col": left}),
        (cot_ref.at[:, pl.ds(0, edge)], cot_x, {"row": above, "col": left}),
    ):
        copy = pltpu.make_async_remote_copy(
            src_ref=source,
            dst_ref=target,
            send_sem=halo_send.at[len(halos)],
            recv_sem=halo_recv.at[len(halos)],
            device_id=device,
            device_id_type=MESH,
        )
        copy.start()
        halos.append(copy)
    send((0, 1, 0, 0), over_core, (1, 1, 0, 0))
    for dy in range(2):
        arrive((0, dy, 1, 0))
        spread(dy, 1)
        send((0, dy, 1, 0), over_core, (1, dy, 1, 0))
    for step in range(1, ring // 2 + 1):
        for dx in range(2):
            for dy in range(2):
                if step < ring // 2 or dy == 0:
                    arrive((0, dy, dx, step))
                    onward_up(dy, dx, step)
                    send((0, dy, dx, step), over_core, (1, dy, dx, step))
                if step < ring // 2 or dy == 1:
                    arrive((0, dy, dx, ring - step))
                    onward_down(dy, dx, step)
                    send((0, dy, dx, ring - step), over_core, (1, dy, dx, ring - step))
    for dz in range(ring):
        for dx in range(2):
            for dy in range(2):
                arrive((1, dy, dx, dz))
    for copy in halos:
        copy.wait_recv()
    for copy in started + halos:
        copy.wait_send()
    for copy in local:
        copy.wait()


def gather_inputs(sizes, qkv_weight, out_weight, cot_block, pix_block):
    rows, cols, dps = sizes
    groups = cols * dps
    edge = (cot_block.shape[0], WIN, cot_block.shape[2])
    cot_type, pix_type = cot_block.dtype, pix_block.dtype
    shapes = [
        ((groups, rows) + qkv_weight.shape, qkv_weight.dtype),
        ((groups, rows) + out_weight.shape, out_weight.dtype),
        (cot_block.shape, cot_type),
        (edge, cot_type),
        (edge, cot_type),
        (pix_block.shape, pix_type),
        (pix_block.shape, pix_type),
        (pix_block.shape, pix_type),
    ]
    return pl.pallas_call(
        functools.partial(gather_kernel, sizes),
        out_shape=[jax.ShapeDtypeStruct(shape, kind) for shape, kind in shapes],
        in_specs=[pl.BlockSpec(memory_space=VMEM)] * 4,
        out_specs=[pl.BlockSpec(memory_space=VMEM)] * 8,
        scratch_shapes=[
            pltpu.SemaphoreType.DMA((4 * rows * groups,)),
            pltpu.SemaphoreType.DMA((2, rows * groups)),
            pltpu.SemaphoreType.DMA((2,)),
            pltpu.SemaphoreType.DMA((6,)),
            pltpu.SemaphoreType.DMA((6,)),
        ],
        compiler_params=pltpu.CompilerParams(
            collective_id=0, has_side_effects=True, vmem_limit_bytes=40 * 2**20
        ),
        name="gather_inputs",
    )(qkv_weight, out_weight, cot_block, pix_block)


def reduce_kernel(
    sizes, grad_ref, small_ref, grad_out, small_out,
    core_g, core_e, made_g, made_e, z_g, z_e, acc_g, acc_e,
    xs_g, xs_e, x_g, x_e, ys_g, y_g, ys_e, y_e, tot_e,
    core_send, core_recv, z_send, z_recv, xy_send, xy_recv, all_send, all_recv,
):
    rows, cols, dps = sizes
    ring = rows // 2
    row, col, dp = lax.axis_index("row"), lax.axis_index("col"), lax.axis_index("dp")
    x, z = row % 2, row // 2
    f32, low = jnp.float32, jnp.bfloat16
    greet_everyone(sizes, row, col, dp)
    other = (col + 1) % 2

    def remote(source, target, send_sem, recv_sem, device):
        copy = pltpu.make_async_remote_copy(
            src_ref=source, dst_ref=target, send_sem=send_sem, recv_sem=recv_sem,
            device_id=device, device_id_type=MESH,
        )
        copy.start()
        return copy

    order = [ring // 2] + [s for s in range(1, ring) if s != ring // 2] + [0]
    across = {}
    for s in order:
        there = ((z + s) % ring) * 2
        across[s] = [
            remote(
                source.at[pl.ds(other * 2, 2), pl.ds(there, 2)], target.at[s],
                core_send.at[i, s], core_recv.at[i, s], {"col": other},
            )
            for i, (source, target) in enumerate(((grad_ref, core_g), (small_ref, core_e)))
        ]
    sent = []
    for s in order:
        for copy in across[s]:
            copy.wait_recv()
        there = ((z + s) % ring) * 2
        for d in range(2):
            for h in range(2):
                total = grad_ref[col * 2 + d, there + h].astype(f32) + core_g[s, d, h].astype(f32)
                small = small_ref[col * 2 + d, there + h] + core_e[s, d, h]
                if s:
                    made_g[s, d, h] = total.astype(low)
                    made_e[s, d, h] = small
                else:
                    acc_g[d, h] = total
                    acc_e[d, h] = small
        if s:
            device = {"row": there + x}
            sent.append(remote(made_g.at[s], z_g.at[s], z_send.at[0, s], z_recv.at[0, s], device))
            sent.append(remote(made_e.at[s], z_e.at[s], z_send.at[1, s], z_recv.at[1, s], device))
    for copy in sent:
        copy.wait_recv()

    def z_sum(d, h):
        total, small = acc_g[d, h], acc_e[d, h]
        for s in range(1, ring):
            total = total + z_g[s, d, h].astype(f32)
            small = small + z_e[s, d, h]
        return total, small

    away = (x + 1) % 2
    for d in range(2):
        total, small = z_sum(d, away)
        xs_g[d] = total.astype(low)
        xs_e[d] = small
    device = {"row": z * 2 + away}
    pair = [
        remote(xs_g, x_g, xy_send.at[0], xy_recv.at[0], device),
        remote(xs_e, x_e, xy_send.at[1], xy_recv.at[1], device),
    ]
    mine, mine_small = z_sum(dp, x)
    far, far_small = z_sum((dp + 1) % 2, x)
    for copy in pair:
        copy.wait_recv()
    ys_g[...] = (far + x_g[(dp + 1) % 2].astype(f32)).astype(low)
    ys_e[...] = far_small + x_e[(dp + 1) % 2]
    device = {"dp": (dp + 1) % 2}
    last = [
        remote(ys_e, y_e, xy_send.at[3], xy_recv.at[3], device),
        remote(ys_g, y_g, xy_send.at[2], xy_recv.at[2], device),
    ]
    mine = mine + x_g[dp].astype(f32)
    mine_small = mine_small + x_e[dp]
    last[0].wait_recv()
    group = col * 2 + dp
    whole = mine_small + y_e[...]
    tot_e[...] = whole
    spread = []
    for r in range(rows):
        for c in range(cols):
            for d in range(dps):
                if r or c or d:
                    index = (r * cols + c) * dps + d
                    spread.append(
                        remote(
                            tot_e, small_out.at[group, row],
                            all_send.at[index], all_recv.at[index],
                            {
                                "row": (row + r) % rows,
                                "col": (col + c) % cols,
                                "dp": (dp + d) % dps,
                            },
                        )
                    )
    small_out[group, row] = whole
    last[1].wait_recv()
    grad_out[...] = mine + y_g[...].astype(f32)
    index = 0
    for r in range(rows):
        for c in range(cols):
            for d in range(dps):
                if r or c or d:
                    place = (r * cols + c) * dps + d
                    source_group = ((col + cols - c) % cols) * dps + (dp + dps - d) % dps
                    pltpu.make_async_remote_copy(
                        src_ref=tot_e,
                        dst_ref=small_out.at[source_group, (row + rows - r) % rows],
                        send_sem=all_send.at[place],
                        recv_sem=all_recv.at[place],
                        device_id={"col": other},
                        device_id_type=MESH,
                    ).wait_recv()
    for s in order:
        for copy in across[s]:
            copy.wait_send()
    for copy in sent + pair + last + spread:
        copy.wait_send()


def reduce_outputs(sizes, grad_blocks, small_blocks):
    rows, cols, dps = sizes
    ring = rows // 2
    big, tiny = grad_blocks.shape[2:], small_blocks.shape[2:]
    f32, low = jnp.float32, jnp.bfloat16
    dma = pltpu.SemaphoreType.DMA
    return pl.pallas_call(
        functools.partial(reduce_kernel, sizes),
        out_shape=[
            jax.ShapeDtypeStruct(big, f32),
            jax.ShapeDtypeStruct(small_blocks.shape, f32),
        ],
        in_specs=[pl.BlockSpec(memory_space=VMEM)] * 2,
        out_specs=[pl.BlockSpec(memory_space=VMEM)] * 2,
        scratch_shapes=[
            VMEM((ring, 2, 2) + big, low), VMEM((ring, 2, 2) + tiny, f32),
            VMEM((ring, 2, 2) + big, low), VMEM((ring, 2, 2) + tiny, f32),
            VMEM((ring, 2, 2) + big, low), VMEM((ring, 2, 2) + tiny, f32),
            VMEM((2, 2) + big, f32), VMEM((2, 2) + tiny, f32),
            VMEM((2,) + big, low), VMEM((2,) + tiny, f32),
            VMEM((2,) + big, low), VMEM((2,) + tiny, f32),
            VMEM(big, low), VMEM(big, low), VMEM(tiny, f32), VMEM(tiny, f32), VMEM(tiny, f32),
            dma((2, ring)), dma((2, ring)), dma((2, ring)), dma((2, ring)),
            dma((4,)), dma((4,)),
            dma((rows * cols * dps,)), dma((rows * cols * dps,)),
        ],
        compiler_params=pltpu.CompilerParams(
            collective_id=1, has_side_effects=True, vmem_limit_bytes=40 * 2**20
        ),
        name="reduce_outputs",
    )(grad_blocks, small_blocks)


def on_device(
    direct,
    sizes,
    pixels,
    cotangent,
    embed_weight,
    embed_bias,
    layer_norm_gain,
    qkv_weight,
    out_weight,
    bias_table,
    rel_index,
    shifts,
):
    images, rows_dev, cols_dev, features = cotangent.shape
    rows, cols, dps = sizes
    head_count, table_size = bias_table.shape
    pix_block, cot_block = pixels[0], cotangent[0]
    row_shift, col_shift = shifts[0, 0], shifts[0, 1]
    if direct:
        qkv_all, out_all, cot_r, cot_c, cot_x, pix_r, pix_c, pix_x = gather_inputs(
            sizes, qkv_weight, out_weight, cot_block, pix_block
        )
        qkv_full = jnp.concatenate(
            [w.reshape(-1, qkv_weight.shape[1]) for w in qkv_all], axis=1
        )
        out_full = jnp.concatenate(
            [w.reshape(-1, out_weight.shape[1]) for w in out_all], axis=1
        )
    else:
        qkv_full, out_full = [
            lax.all_gather(
                lax.all_gather(w, "row", axis=0, tiled=True), ("col", "dp"), axis=1, tiled=True
            )
            for w in (qkv_weight, out_weight)
        ]
        pix_r, cot_r = from_behind((pix_block, cot_block), "row", -1)
        pix_c, cot_c = from_behind((pix_block, cot_block[:, :WIN]), "col", -1)
        pix_x, cot_x = from_behind((pix_c, cot_c), "row", -1)
    wide_pix = jnp.concatenate(
        [
            jnp.concatenate([pix_block, pix_c[:, :, : WIN * PATCH]], axis=2),
            jnp.concatenate([pix_r, pix_x[:, :, : WIN * PATCH]], axis=2),
        ],
        axis=1,
    )
    wide_cot = jnp.concatenate(
        [
            jnp.concatenate([cot_block, cot_c], axis=1),
            jnp.concatenate([cot_r, cot_x], axis=1),
        ],
        axis=0,
    )
    wide_patches = make_patches(wide_pix[None])[0]
    patches = lax.dynamic_slice(
        wide_patches, (row_shift, col_shift, 0), (rows_dev, cols_dev, wide_patches.shape[2])
    )
    shifted_cot = lax.dynamic_slice(
        wide_cot, (row_shift, col_shift, 0), (rows_dev, cols_dev, features)
    )
    patch_rows = window_split(patches).reshape(-1, patches.shape[2])
    cot_flat = window_split(shifted_cot).reshape(-1, features)
    grid_rows, grid_cols = rows_dev * rows, cols_dev * cols
    row_ids = lax.axis_index("row") * rows_dev + jnp.arange(rows_dev, dtype=jnp.int32)
    col_ids = lax.axis_index("col") * cols_dev + jnp.arange(cols_dev, dtype=jnp.int32)
    row_part = (row_ids >= grid_rows - row_shift).astype(jnp.int32)
    col_part = (col_ids >= grid_cols - col_shift).astype(jnp.int32)
    region = 2 * row_part[:, None] + col_part[None, :]
    labels = window_split(region[:, :, None])[:, :, 0]
    selector = (
        rel_index.reshape(-1)[:, None] == jnp.arange(table_size, dtype=jnp.int32)[None, :]
    ).astype(jnp.float32)
    bias_full = jnp.dot(selector, bias_table.T, precision=lax.Precision.HIGHEST).T.reshape(
        head_count, WIN * WIN, WIN * WIN
    )
    cells = embed_cells(patch_rows, embed_weight, embed_bias)
    stored_residuals, attended = attend_forward(
        cells.reshape(-1, WIN * WIN, features), labels, layer_norm_gain, qkv_full, bias_full
    )
    d_attended = lax.dot_general(
        cot_flat, out_full, (((1,), (1,)), ((), ())), preferred_element_type=jnp.float32
    ).astype(jnp.bfloat16)
    d_rows, gain_contribution, table_part = attend_backward(
        stored_residuals, d_attended, layer_norm_gain, qkv_full
    )
    table_grad = jnp.dot(
        table_part.reshape(head_count, -1), selector, precision=lax.Precision.HIGHEST
    )
    contract = (((0,), (0,)), ((), ()))
    back_rows = jnp.concatenate([cot_flat, d_rows], axis=0)
    embed_grad = lax.dot_general(
        jnp.concatenate([patch_rows, patch_rows], axis=0),
        back_rows,
        contract,
        preferred_element_type=jnp.float32,
    )
    bias_grad = jnp.sum(back_rows, axis=0, dtype=jnp.float32)
    if not direct:
        partial_rows = lax.psum_scatter(
            lax.dot_general(attended, cot_flat, contract, preferred_element_type=jnp.float32),
            "row",
            scatter_dimension=0,
            tiled=True,
        )
        out_weight_grad = lax.psum_scatter(
            partial_rows, ("col", "dp"), scatter_dimension=1, tiled=True
        )
        totals = lax.psum(
            (embed_grad, bias_grad, gain_contribution, table_grad), ("row", "col", "dp")
        )
        return (out_weight_grad,) + totals
    groups = cols * dps
    cot_groups = cot_flat.reshape(-1, groups, features // groups)
    grad_blocks = jnp.stack(
        [
            lax.dot_general(
                attended, cot_groups[:, k], contract, preferred_element_type=jnp.float32
            ).astype(jnp.bfloat16)
            for k in range(groups)
        ]
    ).reshape((groups, rows) + out_weight.shape)
    pieces = (embed_grad, bias_grad, gain_contribution, table_grad)
    flat = jnp.concatenate([piece.reshape(-1) for piece in pieces])
    unit = groups * rows * 2048
    flat = jnp.pad(flat, (0, -flat.shape[0] % unit))
    out_weight_grad, small = reduce_outputs(
        sizes, grad_blocks, flat.reshape(groups, rows, -1, 256)
    )
    small = small.reshape(-1)
    totals, start = [], 0
    for piece in pieces:
        totals.append(small[start : start + piece.size].reshape(piece.shape))
        start += piece.size
    return (out_weight_grad,) + tuple(totals)


def solution(mesh):
    sizes = tuple(mesh.shape[name] for name in ("row", "col", "dp"))
    direct = sizes[1:] == (2, 2) and sizes[0] == 8
    return jax.shard_map(
        functools.partial(on_device, direct, sizes),
        mesh=mesh,
        in_specs=(
            P("dp", None, "row", "col"),
            P("dp", "row", "col", None),
            P(),
            P(),
            P(),
            P("row", ("col", "dp")),
            P("row", ("col", "dp")),
            P(),
            P(),
            P("dp", None),
        ),
        out_specs=(P("row", ("col", "dp")), P(), P(), P(), P()),
        check_vma=False,
    )
```

```python
import functools

import jax
import jax.numpy as jnp
from jax import lax
from jax.experimental import pallas as pl
from jax.experimental.pallas import tpu as pltpu
from jax.sharding import PartitionSpec as P

WIN = 8
PATCH = 4


norm_epsilon = 1e-05


def from_behind(value, axis, steps):
    count = lax.axis_size(axis)
    pairs = [(source, (source + steps) % count) for source in range(count)]
    return lax.ppermute(value, axis, pairs)


def make_patches(pixel_block):
    images, channels, pixel_rows, pixel_cols = pixel_block.shape
    grid_rows = pixel_rows // PATCH
    grid_cols = pixel_cols // PATCH
    shaped = pixel_block.reshape(images, channels, grid_rows, PATCH, grid_cols, PATCH)
    return shaped.transpose(0, 2, 4, 1, 3, 5).reshape(
        images, grid_rows, grid_cols, channels * PATCH * PATCH
    )


def embed_cells(patches, embed_weight, embed_bias):
    return (jnp.dot(patches, embed_weight, preferred_element_type=jnp.float32) + embed_bias).astype(
        jnp.bfloat16
    )


def window_split(block):
    rows_all, cols_all, features = block.shape
    shaped = block.reshape(rows_all // WIN, WIN, cols_all // WIN, WIN, features)
    return shaped.transpose(0, 2, 1, 3, 4).reshape(-1, WIN * WIN, features)


def window_join(windows, rows_all, cols_all):
    features = windows.shape[-1]
    shaped = windows.reshape(rows_all // WIN, cols_all // WIN, WIN, WIN, features)
    return shaped.transpose(0, 2, 1, 3, 4).reshape(rows_all, cols_all, features)

def attend_forward(cell_windows, labels, layer_norm_gain, qkv_full, bias_full):
    window_count, cell_count, features = cell_windows.shape
    head_count = bias_full.shape[0]
    inner_width = qkv_full.shape[1] // 3
    head_size = inner_width // head_count
    score_scale = head_size ** (-0.5)
    flat_rows = cell_windows.reshape(-1, features).astype(jnp.float32)
    average = jnp.mean(flat_rows, axis=-1, keepdims=True)
    centered_input = flat_rows - average
    inverse_deviation = lax.rsqrt(
        jnp.mean(centered_input * centered_input, axis=-1, keepdims=True) + norm_epsilon
    )
    standardized_rows = centered_input * inverse_deviation
    normalized_rows = (standardized_rows * layer_norm_gain).astype(jnp.bfloat16)
    projected = jnp.dot(normalized_rows, qkv_full, preferred_element_type=jnp.float32).astype(
        jnp.bfloat16
    )
    head_shape = (window_count, cell_count, head_count, head_size)
    query_rows = projected[:, :inner_width].reshape(head_shape)
    key_vectors = projected[:, inner_width : 2 * inner_width].reshape(head_shape)
    value_rows = projected[:, 2 * inner_width :].reshape(head_shape)
    scores = (
        jnp.einsum("wmhd,wnhd->whmn", query_rows, key_vectors, preferred_element_type=jnp.float32)
        * score_scale
        + bias_full[None]
    )
    same_region = labels[:, None, :, None] == labels[:, None, None, :]
    scores = jnp.where(same_region, scores, -1e30)
    row_peak = jnp.max(scores, axis=-1, keepdims=True)
    exp_scores = jnp.exp(scores - row_peak)
    attention_weights = exp_scores / jnp.sum(exp_scores, axis=-1, keepdims=True)
    reduced_probability = attention_weights.astype(jnp.bfloat16)
    attended = jnp.einsum(
        "whmn,wnhd->wmhd", reduced_probability, value_rows, preferred_element_type=jnp.float32
    ).astype(jnp.bfloat16)
    stored_residuals = (
        standardized_rows,
        inverse_deviation,
        query_rows,
        key_vectors,
        value_rows,
        attention_weights,
        reduced_probability,
    )
    return (stored_residuals, attended.reshape(-1, inner_width))


def attend_backward(stored_residuals, d_attended, layer_norm_gain, qkv_full):
    (
        standardized_rows,
        inverse_deviation,
        query_rows,
        key_vectors,
        value_rows,
        attention_weights,
        reduced_probability,
    ) = stored_residuals
    head_shape = query_rows.shape
    score_scale = head_shape[3] ** (-0.5)
    total_row_count = standardized_rows.shape[0]
    inner_width = head_shape[2] * head_shape[3]
    d_heads = d_attended.reshape(head_shape)
    d_prob = jnp.einsum("wmhd,wnhd->whmn", d_heads, value_rows, preferred_element_type=jnp.float32)
    d_values = jnp.einsum(
        "whmn,wmhd->wnhd", reduced_probability, d_heads, preferred_element_type=jnp.float32
    ).astype(jnp.bfloat16)
    d_scores = attention_weights * (
        d_prob - jnp.sum(attention_weights * d_prob, axis=-1, keepdims=True)
    )
    table_part = jnp.sum(d_scores, axis=0)
    d_low = d_scores.astype(jnp.bfloat16)
    d_queries = (
        jnp.einsum("whmn,wnhd->wmhd", d_low, key_vectors, preferred_element_type=jnp.float32)
        * score_scale
    ).astype(jnp.bfloat16)
    d_keys = (
        jnp.einsum("whmn,wmhd->wnhd", d_low, query_rows, preferred_element_type=jnp.float32)
        * score_scale
    ).astype(jnp.bfloat16)
    d_projected = jnp.concatenate(
        [
            d_queries.reshape(total_row_count, inner_width),
            d_keys.reshape(total_row_count, inner_width),
            d_values.reshape(total_row_count, inner_width),
        ],
        axis=1,
    )
    normalized_gradient = lax.dot_general(
        d_projected, qkv_full, (((1,), (1,)), ((), ())), preferred_element_type=jnp.float32
    )
    gain_contribution = jnp.sum(normalized_gradient * standardized_rows, axis=0)
    scaled_rows = normalized_gradient * layer_norm_gain
    branch_gradient = inverse_deviation * (
        scaled_rows
        - jnp.mean(scaled_rows, axis=-1, keepdims=True)
        - standardized_rows * jnp.mean(scaled_rows * standardized_rows, axis=-1, keepdims=True)
    )
    return (branch_gradient.astype(jnp.bfloat16), gain_contribution, table_part)


MESH = pl.DeviceIdType.MESH
VMEM = pltpu.VMEM


def greet_everyone(sizes, row, col, dp):
    rows, cols, dps = sizes
    barrier = pltpu.get_barrier_semaphore()
    others = 0
    for r in range(rows):
        for c in range(cols):
            for d in range(dps):
                if r or c or d:
                    others += 1
                    pl.semaphore_signal(
                        barrier,
                        inc=1,
                        device_id={
                            "row": (row + r) % rows,
                            "col": (col + c) % cols,
                            "dp": (dp + d) % dps,
                        },
                        device_id_type=MESH,
                    )
    pl.semaphore_wait(barrier, others)


def gather_kernel(
    sizes, qkv_ref, out_ref, cot_ref, pix_ref,
    qkv_all, out_all, cot_r, cot_c, cot_x, pix_r, pix_c, pix_x,
    send_sem, recv_sem, own_sem, halo_send, halo_recv,
):
    rows, cols, _ = sizes
    ring = rows // 2
    row, col, dp = lax.axis_index("row"), lax.axis_index("col"), lax.axis_index("dp")
    x, z = row % 2, row // 2
    greet_everyone(sizes, row, col, dp)
    gathered = (qkv_all, out_all)
    own = (qkv_ref, out_ref)
    started = []

    def slot(array, ident):
        flag, dy, dx, dz = ident
        column = (col + flag) % 2
        which_row = ((z - dz + ring) % ring) * 2 + (x + dx) % 2
        return gathered[array].at[column * 2 + (dp + dy) % 2, which_row]

    def semaphore(array, ident):
        flag, dy, dx, dz = ident
        return recv_sem.at[array, ((flag * 2 + dy) * 2 + dx) * ring + dz]

    def send(ident, device, landing):
        for array in range(2):
            source = own[array] if ident == (0, 0, 0, 0) else slot(array, ident)
            copy = pltpu.make_async_remote_copy(
                src_ref=source,
                dst_ref=slot(array, ident),
                send_sem=send_sem.at[len(started)],
                recv_sem=semaphore(array, landing),
                device_id=device,
                device_id_type=MESH,
            )
            copy.start()
            started.append(copy)

    def arrive(ident):
        for array in range(2):
            pltpu.make_async_remote_copy(
                src_ref=slot(array, ident),
                dst_ref=slot(array, ident),
                send_sem=send_sem.at[0],
                recv_sem=semaphore(array, ident),
                device_id={"col": (col + 1) % 2},
                device_id_type=MESH,
            ).wait_recv()

    over_y = {"dp": (dp + 1) % 2}
    over_x = {"row": z * 2 + (x + 1) % 2}
    up = {"row": ((z + 1) % ring) * 2 + x}
    down = {"row": ((z + ring - 1) % ring) * 2 + x}
    over_core = {"col": (col + 1) % 2}

    def onward_up(dy, dx, dz):
        if dz + 1 < ring // 2 or (dz + 1 == ring // 2 and dy == 0):
            send((0, dy, dx, dz), up, (0, dy, dx, dz + 1))

    def onward_down(dy, dx, back):
        if back + 1 < ring // 2 or (back + 1 == ring // 2 and dy == 1):
            send((0, dy, dx, (ring - back) % ring), down, (0, dy, dx, ring - back - 1))

    def spread(dy, dx):
        onward_up(dy, dx, 0)
        onward_down(dy, dx, 0)

    send((0, 0, 0, 0), over_y, (0, 1, 0, 0))
    send((0, 0, 0, 0), over_x, (0, 0, 1, 0))
    spread(0, 0)
    send((0, 0, 0, 0), over_core, (1, 0, 0, 0))
    local = [
        pltpu.make_async_copy(own[array], slot(array, (0, 0, 0, 0)), own_sem.at[array])
        for array in range(2)
    ]
    for copy in local:
        copy.start()
    arrive((0, 1, 0, 0))
    send((0, 1, 0, 0), over_x, (0, 1, 1, 0))
    spread(1, 0)
    above = (row + rows - 1) % rows
    left = (col + cols - 1) % cols
    edge = cot_c.shape[1]
    halos = []
    for source, target, device in (
        (pix_ref, pix_r, {"row": above}),
        (pix_ref, pix_c, {"col": left}),
        (pix_ref, pix_x, {"row": above, "col": left}),
        (cot_ref, cot_r, {"row": above}),
        (cot_ref.at[:, pl.ds(0, edge)], cot_c, {"col": left}),
        (cot_ref.at[:, pl.ds(0, edge)], cot_x, {"row": above, "col": left}),
    ):
        copy = pltpu.make_async_remote_copy(
            src_ref=source,
            dst_ref=target,
            send_sem=halo_send.at[len(halos)],
            recv_sem=halo_recv.at[len(halos)],
            device_id=device,
            device_id_type=MESH,
        )
        copy.start()
        halos.append(copy)
    send((0, 1, 0, 0), over_core, (1, 1, 0, 0))
    for dy in range(2):
        arrive((0, dy, 1, 0))
        spread(dy, 1)
        send((0, dy, 1, 0), over_core, (1, dy, 1, 0))
    for step in range(1, ring // 2 + 1):
        for dx in range(2):
            for dy in range(2):
                if step < ring // 2 or dy == 0:
                    arrive((0, dy, dx, step))
                    onward_up(dy, dx, step)
                    send((0, dy, dx, step), over_core, (1, dy, dx, step))
                if step < ring // 2 or dy == 1:
                    arrive((0, dy, dx, ring - step))
                    onward_down(dy, dx, step)
                    send((0, dy, dx, ring - step), over_core, (1, dy, dx, ring - step))
    for dz in range(ring):
        for dx in range(2):
            for dy in range(2):
                arrive((1, dy, dx, dz))
    for copy in halos:
        copy.wait_recv()
    for copy in started + halos:
        copy.wait_send()
    for copy in local:
        copy.wait()


def gather_inputs(sizes, qkv_weight, out_weight, cot_block, pix_block):
    rows, cols, dps = sizes
    groups = cols * dps
    edge = (cot_block.shape[0], WIN, cot_block.shape[2])
    cot_type, pix_type = cot_block.dtype, pix_block.dtype
    shapes = [
        ((groups, rows) + qkv_weight.shape, qkv_weight.dtype),
        ((groups, rows) + out_weight.shape, out_weight.dtype),
        (cot_block.shape, cot_type),
        (edge, cot_type),
        (edge, cot_type),
        (pix_block.shape, pix_type),
        (pix_block.shape, pix_type),
        (pix_block.shape, pix_type),
    ]
    return pl.pallas_call(
        functools.partial(gather_kernel, sizes),
        out_shape=[jax.ShapeDtypeStruct(shape, kind) for shape, kind in shapes],
        in_specs=[pl.BlockSpec(memory_space=VMEM)] * 4,
        out_specs=[pl.BlockSpec(memory_space=VMEM)] * 8,
        scratch_shapes=[
            pltpu.SemaphoreType.DMA((4 * rows * groups,)),
            pltpu.SemaphoreType.DMA((2, rows * groups)),
            pltpu.SemaphoreType.DMA((2,)),
            pltpu.SemaphoreType.DMA((6,)),
            pltpu.SemaphoreType.DMA((6,)),
        ],
        compiler_params=pltpu.CompilerParams(
            collective_id=0, has_side_effects=True, vmem_limit_bytes=40 * 2**20
        ),
        name="gather_inputs",
    )(qkv_weight, out_weight, cot_block, pix_block)


def reduce_kernel(
    sizes, grad_ref, small_ref, grad_out, small_out,
    core_g, core_e, made_g, made_e, z_g, z_e, acc_g, acc_e,
    xs_g, xs_e, x_g, x_e, ys_g, y_g, ys_e, y_e, tot_e,
    core_send, core_recv, z_send, z_recv, xy_send, xy_recv, all_send, all_recv,
):
    rows, cols, dps = sizes
    ring = rows // 2
    row, col, dp = lax.axis_index("row"), lax.axis_index("col"), lax.axis_index("dp")
    x, z = row % 2, row // 2
    f32, low = jnp.float32, jnp.bfloat16
    greet_everyone(sizes, row, col, dp)
    other = (col + 1) % 2

    def remote(source, target, send_sem, recv_sem, device):
        copy = pltpu.make_async_remote_copy(
            src_ref=source, dst_ref=target, send_sem=send_sem, recv_sem=recv_sem,
            device_id=device, device_id_type=MESH,
        )
        copy.start()
        return copy

    order = [ring // 2] + [s for s in range(1, ring) if s != ring // 2] + [0]
    across = {}
    for s in order:
        there = ((z + s) % ring) * 2
        across[s] = [
            remote(
                source.at[pl.ds(other * 2, 2), pl.ds(there, 2)], target.at[s],
                core_send.at[i, s], core_recv.at[i, s], {"col": other},
            )
            for i, (source, target) in enumerate(((grad_ref, core_g), (small_ref, core_e)))
        ]
    sent = []
    for s in order:
        for copy in across[s]:
            copy.wait_recv()
        there = ((z + s) % ring) * 2
        for d in range(2):
            for h in range(2):
                total = grad_ref[col * 2 + d, there + h].astype(f32) + core_g[s, d, h].astype(f32)
                small = small_ref[col * 2 + d, there + h] + core_e[s, d, h]
                if s:
                    made_g[s, d, h] = total.astype(low)
                    made_e[s, d, h] = small
                else:
                    acc_g[d, h] = total
                    acc_e[d, h] = small
        if s:
            device = {"row": there + x}
            sent.append(remote(made_g.at[s], z_g.at[s], z_send.at[0, s], z_recv.at[0, s], device))
            sent.append(remote(made_e.at[s], z_e.at[s], z_send.at[1, s], z_recv.at[1, s], device))
    for copy in sent:
        copy.wait_recv()

    def z_sum(d, h):
        total, small = acc_g[d, h], acc_e[d, h]
        for s in range(1, ring):
            total = total + z_g[s, d, h].astype(f32)
            small = small + z_e[s, d, h]
        return total, small

    away = (x + 1) % 2
    for d in range(2):
        total, small = z_sum(d, away)
        xs_g[d] = total.astype(low)
        xs_e[d] = small
    device = {"row": z * 2 + away}
    pair = [
        remote(xs_g, x_g, xy_send.at[0], xy_recv.at[0], device),
        remote(xs_e, x_e, xy_send.at[1], xy_recv.at[1], device),
    ]
    mine, mine_small = z_sum(dp, x)
    far, far_small = z_sum((dp + 1) % 2, x)
    for copy in pair:
        copy.wait_recv()
    ys_g[...] = (far + x_g[(dp + 1) % 2].astype(f32)).astype(low)
    ys_e[...] = far_small + x_e[(dp + 1) % 2]
    device = {"dp": (dp + 1) % 2}
    last = [
        remote(ys_e, y_e, xy_send.at[3], xy_recv.at[3], device),
        remote(ys_g, y_g, xy_send.at[2], xy_recv.at[2], device),
    ]
    mine = mine + x_g[dp].astype(f32)
    mine_small = mine_small + x_e[dp]
    last[0].wait_recv()
    group = col * 2 + dp
    whole = mine_small + y_e[...]
    tot_e[...] = whole
    spread = []
    for r in range(rows):
        for c in range(cols):
            for d in range(dps):
                if r or c or d:
                    index = (r * cols + c) * dps + d
                    spread.append(
                        remote(
                            tot_e, small_out.at[group, row],
                            all_send.at[index], all_recv.at[index],
                            {
                                "row": (row + r) % rows,
                                "col": (col + c) % cols,
                                "dp": (dp + d) % dps,
                            },
                        )
                    )
    small_out[group, row] = whole
    last[1].wait_recv()
    grad_out[...] = mine + y_g[...].astype(f32)
    index = 0
    for r in range(rows):
        for c in range(cols):
            for d in range(dps):
                if r or c or d:
                    place = (r * cols + c) * dps + d
                    source_group = ((col + cols - c) % cols) * dps + (dp + dps - d) % dps
                    pltpu.make_async_remote_copy(
                        src_ref=tot_e,
                        dst_ref=small_out.at[source_group, (row + rows - r) % rows],
                        send_sem=all_send.at[place],
                        recv_sem=all_recv.at[place],
                        device_id={"col": other},
                        device_id_type=MESH,
                    ).wait_recv()
    for s in order:
        for copy in across[s]:
            copy.wait_send()
    for copy in sent + pair + last + spread:
        copy.wait_send()


def reduce_outputs(sizes, grad_blocks, small_blocks):
    rows, cols, dps = sizes
    ring = rows // 2
    big, tiny = grad_blocks.shape[2:], small_blocks.shape[2:]
    f32, low = jnp.float32, jnp.bfloat16
    dma = pltpu.SemaphoreType.DMA
    return pl.pallas_call(
        functools.partial(reduce_kernel, sizes),
        out_shape=[
            jax.ShapeDtypeStruct(big, f32),
            jax.ShapeDtypeStruct(small_blocks.shape, f32),
        ],
        in_specs=[pl.BlockSpec(memory_space=VMEM)] * 2,
        out_specs=[pl.BlockSpec(memory_space=VMEM)] * 2,
        scratch_shapes=[
            VMEM((ring, 2, 2) + big, low), VMEM((ring, 2, 2) + tiny, f32),
            VMEM((ring, 2, 2) + big, low), VMEM((ring, 2, 2) + tiny, f32),
            VMEM((ring, 2, 2) + big, low), VMEM((ring, 2, 2) + tiny, f32),
            VMEM((2, 2) + big, f32), VMEM((2, 2) + tiny, f32),
            VMEM((2,) + big, low), VMEM((2,) + tiny, f32),
            VMEM((2,) + big, low), VMEM((2,) + tiny, f32),
            VMEM(big, low), VMEM(big, low), VMEM(tiny, f32), VMEM(tiny, f32), VMEM(tiny, f32),
            dma((2, ring)), dma((2, ring)), dma((2, ring)), dma((2, ring)),
            dma((4,)), dma((4,)),
            dma((rows * cols * dps,)), dma((rows * cols * dps,)),
        ],
        compiler_params=pltpu.CompilerParams(
            collective_id=1, has_side_effects=True, vmem_limit_bytes=40 * 2**20
        ),
        name="reduce_outputs",
    )(grad_blocks, small_blocks)


def block_kernel(
    heads, patch_ref, cot_ref, embed_ref, ebias_ref, gain_ref, qkv_ref, out_ref, bias_ref,
    tag_col_ref, tag_row_ref,
    grad_ref, egrad_ref, bgrad_ref, ggrad_ref, table_ref,
    xhat_ref, proj_ref, datt_ref, att_ref, dproj_ref,
):
    f32, low = jnp.float32, jnp.bfloat16
    groups = qkv_ref.shape[0]
    share, part = qkv_ref.shape[2], out_ref.shape[2]
    inner = out_ref.shape[1]
    size = inner // heads
    cells, features = cot_ref.shape
    repeat = cells // bias_ref.shape[1]
    scale = size ** (-0.5)
    nt = (((1,), (1,)), ((), ()))
    tn = (((0,), (0,)), ((), ()))

    def dot(a, b, dims=(((1,), (0,)), ((), ()))):
        return lax.dot_general(a, b, dims, preferred_element_type=f32)

    gain = gain_ref[...]
    rows = (dot(patch_ref[...], embed_ref[...]) + ebias_ref[...]).astype(low).astype(f32)
    centered = rows - jnp.mean(rows, axis=1, keepdims=True)
    inv_std = lax.rsqrt(jnp.mean(centered * centered, axis=1, keepdims=True) + norm_epsilon)
    xhat_ref[...] = centered * inv_std
    normed = (xhat_ref[...] * gain).astype(low)
    total = None
    for k in range(groups):
        proj_ref[:, k * share : (k + 1) * share] = dot(normed, qkv_ref[k]).astype(low)
        term = dot(cot_ref[:, k * part : (k + 1) * part], out_ref[k], nt)
        total = term if total is None else total + term
    datt_ref[...] = total.astype(low)
    allowed = tag_col_ref[...] == tag_row_ref[...]
    for h in range(heads):
        q = proj_ref[:, h * size : (h + 1) * size]
        key = proj_ref[:, inner + h * size : inner + (h + 1) * size]
        v = proj_ref[:, 2 * inner + h * size : 2 * inner + (h + 1) * size]
        da = datt_ref[:, h * size : (h + 1) * size]
        bias = jnp.concatenate([bias_ref[h]] * repeat, axis=0)
        scores = jnp.where(allowed, dot(q, key, nt) * scale + bias, -1e30)
        weights = jnp.exp(scores - jnp.max(scores, axis=1, keepdims=True))
        prob = weights / jnp.sum(weights, axis=1, keepdims=True)
        prob_low = prob.astype(low)
        att_ref[:, h * size : (h + 1) * size] = dot(prob_low, v).astype(low)
        d_prob = dot(da, v, nt)
        d_scores = prob * (d_prob - jnp.sum(prob * d_prob, axis=1, keepdims=True))
        folded = d_scores[: cells // repeat]
        for w in range(1, repeat):
            folded = folded + d_scores[w * (cells // repeat) : (w + 1) * (cells // repeat)]
        table_ref[h] = folded
        d_low = d_scores.astype(low)
        dproj_ref[:, h * size : (h + 1) * size] = (dot(d_low, key) * scale).astype(low)
        dproj_ref[:, inner + h * size : inner + (h + 1) * size] = (
            dot(d_low, q, tn) * scale
        ).astype(low)
        dproj_ref[:, 2 * inner + h * size : 2 * inner + (h + 1) * size] = dot(
            prob_low, da, tn
        ).astype(low)
    d_normed = None
    for k in range(groups):
        grad_ref[k] = dot(att_ref[...], cot_ref[:, k * part : (k + 1) * part], tn).astype(low)
        term = dot(dproj_ref[:, k * share : (k + 1) * share], qkv_ref[k], nt)
        d_normed = term if d_normed is None else d_normed + term
    xhat = xhat_ref[...]
    ggrad_ref[...] = jnp.sum(d_normed * xhat, axis=0, keepdims=True)
    g = d_normed * gain
    branch = inv_std * (
        g
        - jnp.mean(g, axis=1, keepdims=True)
        - xhat * jnp.mean(g * xhat, axis=1, keepdims=True)
    )
    branch = branch.astype(low)
    patches = patch_ref[...]
    egrad_ref[...] = dot(patches, cot_ref[...], tn) + dot(patches, branch, tn)
    bgrad_ref[...] = jnp.sum(
        cot_ref[...].astype(f32) + branch.astype(f32), axis=0, keepdims=True
    )


def block_grads(patch_rows, cot_rows, embed_weight, embed_bias, gain, qkv_all, out_all, bias_full, labels):
    f32, low = jnp.float32, jnp.bfloat16
    cells, features = cot_rows.shape
    heads, span = bias_full.shape[:2]
    inner = out_all.shape[1]
    windows = cells // span
    tags = (labels + 4 * jnp.arange(windows, dtype=jnp.int32)[:, None]).reshape(-1)
    vmem = pl.BlockSpec(memory_space=VMEM)
    shapes = [
        (out_all.shape, low),
        ((patch_rows.shape[1], features), f32),
        ((1, features), f32),
        ((1, features), f32),
        ((heads, span, cells), f32),
    ]
    grad, egrad, bgrad, ggrad, table = pl.pallas_call(
        functools.partial(block_kernel, heads),
        out_shape=[jax.ShapeDtypeStruct(shape, kind) for shape, kind in shapes],
        in_specs=[vmem] * 10,
        out_specs=[vmem] * 5,
        scratch_shapes=[
            VMEM((cells, features), f32),
            VMEM((cells, 3 * inner), low),
            VMEM((cells, inner), low),
            VMEM((cells, inner), low),
            VMEM((cells, 3 * inner), low),
        ],
        compiler_params=pltpu.CompilerParams(vmem_limit_bytes=48 * 2**20),
        name="block_grads",
    )(
        patch_rows, cot_rows, embed_weight, embed_bias[None], gain[None], qkv_all, out_all,
        jnp.concatenate([bias_full] * windows, axis=2), tags[:, None], tags[None],
    )
    table_part = table.reshape(heads, span, windows, span).sum(axis=2)
    return grad, egrad, bgrad[0], ggrad[0], table_part


def on_device(
    direct,
    sizes,
    pixels,
    cotangent,
    embed_weight,
    embed_bias,
    layer_norm_gain,
    qkv_weight,
    out_weight,
    bias_table,
    rel_index,
    shifts,
):
    images, rows_dev, cols_dev, features = cotangent.shape
    rows, cols, dps = sizes
    head_count, table_size = bias_table.shape
    pix_block, cot_block = pixels[0], cotangent[0]
    row_shift, col_shift = shifts[0, 0], shifts[0, 1]
    if direct:
        qkv_all, out_all, cot_r, cot_c, cot_x, pix_r, pix_c, pix_x = gather_inputs(
            sizes, qkv_weight, out_weight, cot_block, pix_block
        )
        qkv_all = qkv_all.reshape(cols * dps, -1, qkv_weight.shape[1])
        out_all = out_all.reshape(cols * dps, -1, out_weight.shape[1])
    else:
        qkv_full, out_full = [
            lax.all_gather(
                lax.all_gather(w, "row", axis=0, tiled=True), ("col", "dp"), axis=1, tiled=True
            )
            for w in (qkv_weight, out_weight)
        ]
        pix_r, cot_r = from_behind((pix_block, cot_block), "row", -1)
        pix_c, cot_c = from_behind((pix_block, cot_block[:, :WIN]), "col", -1)
        pix_x, cot_x = from_behind((pix_c, cot_c), "row", -1)
    wide_pix = jnp.concatenate(
        [
            jnp.concatenate([pix_block, pix_c[:, :, : WIN * PATCH]], axis=2),
            jnp.concatenate([pix_r, pix_x[:, :, : WIN * PATCH]], axis=2),
        ],
        axis=1,
    )
    wide_cot = jnp.concatenate(
        [
            jnp.concatenate([cot_block, cot_c], axis=1),
            jnp.concatenate([cot_r, cot_x], axis=1),
        ],
        axis=0,
    )
    wide_patches = make_patches(wide_pix[None])[0]
    patches = lax.dynamic_slice(
        wide_patches, (row_shift, col_shift, 0), (rows_dev, cols_dev, wide_patches.shape[2])
    )
    shifted_cot = lax.dynamic_slice(
        wide_cot, (row_shift, col_shift, 0), (rows_dev, cols_dev, features)
    )
    patch_rows = window_split(patches).reshape(-1, patches.shape[2])
    cot_flat = window_split(shifted_cot).reshape(-1, features)
    grid_rows, grid_cols = rows_dev * rows, cols_dev * cols
    row_ids = lax.axis_index("row") * rows_dev + jnp.arange(rows_dev, dtype=jnp.int32)
    col_ids = lax.axis_index("col") * cols_dev + jnp.arange(cols_dev, dtype=jnp.int32)
    row_part = (row_ids >= grid_rows - row_shift).astype(jnp.int32)
    col_part = (col_ids >= grid_cols - col_shift).astype(jnp.int32)
    region = 2 * row_part[:, None] + col_part[None, :]
    labels = window_split(region[:, :, None])[:, :, 0]
    selector = (
        rel_index.reshape(-1)[:, None] == jnp.arange(table_size, dtype=jnp.int32)[None, :]
    ).astype(jnp.float32)
    bias_full = jnp.dot(selector, bias_table.T, precision=lax.Precision.HIGHEST).T.reshape(
        head_count, WIN * WIN, WIN * WIN
    )
    contract = (((0,), (0,)), ((), ()))
    if not direct:
        cells = embed_cells(patch_rows, embed_weight, embed_bias)
        stored_residuals, attended = attend_forward(
            cells.reshape(-1, WIN * WIN, features), labels, layer_norm_gain, qkv_full, bias_full
        )
        d_attended = lax.dot_general(
            cot_flat, out_full, (((1,), (1,)), ((), ())), preferred_element_type=jnp.float32
        ).astype(jnp.bfloat16)
        d_rows, gain_contribution, table_part = attend_backward(
            stored_residuals, d_attended, layer_norm_gain, qkv_full
        )
        table_grad = jnp.dot(
            table_part.reshape(head_count, -1), selector, precision=lax.Precision.HIGHEST
        )
        contract = (((0,), (0,)), ((), ()))
        back_rows = jnp.concatenate([cot_flat, d_rows], axis=0)
        embed_grad = lax.dot_general(
            jnp.concatenate([patch_rows, patch_rows], axis=0),
            back_rows,
            contract,
            preferred_element_type=jnp.float32,
        )
        bias_grad = jnp.sum(back_rows, axis=0, dtype=jnp.float32)
        partial_rows = lax.psum_scatter(
            lax.dot_general(attended, cot_flat, contract, preferred_element_type=jnp.float32),
            "row",
            scatter_dimension=0,
            tiled=True,
        )
        out_weight_grad = lax.psum_scatter(
            partial_rows, ("col", "dp"), scatter_dimension=1, tiled=True
        )
        totals = lax.psum(
            (embed_grad, bias_grad, gain_contribution, table_grad), ("row", "col", "dp")
        )
        return (out_weight_grad,) + totals
    groups = cols * dps
    grad_blocks, embed_grad, bias_grad, gain_contribution, table_part = block_grads(
        patch_rows, cot_flat, embed_weight, embed_bias, layer_norm_gain, qkv_all, out_all,
        bias_full, labels,
    )
    grad_blocks = grad_blocks.reshape((groups, rows) + out_weight.shape)
    table_grad = jnp.dot(
        table_part.reshape(head_count, -1), selector, precision=lax.Precision.HIGHEST
    )
    pieces = (embed_grad, bias_grad, gain_contribution, table_grad)
    flat = jnp.concatenate([piece.reshape(-1) for piece in pieces])
    unit = groups * rows * 2048
    flat = jnp.pad(flat, (0, -flat.shape[0] % unit))
    out_weight_grad, small = reduce_outputs(
        sizes, grad_blocks, flat.reshape(groups, rows, -1, 256)
    )
    small = small.reshape(-1)
    totals, start = [], 0
    for piece in pieces:
        totals.append(small[start : start + piece.size].reshape(piece.shape))
        start += piece.size
    return (out_weight_grad,) + tuple(totals)


def solution(mesh):
    sizes = tuple(mesh.shape[name] for name in ("row", "col", "dp"))
    direct = sizes[1:] == (2, 2) and sizes[0] == 8
    return jax.shard_map(
        functools.partial(on_device, direct, sizes),
        mesh=mesh,
        in_specs=(
            P("dp", None, "row", "col"),
            P("dp", "row", "col", None),
            P(),
            P(),
            P(),
            P("row", ("col", "dp")),
            P("row", ("col", "dp")),
            P(),
            P(),
            P("dp", None),
        ),
        out_specs=(P("row", ("col", "dp")), P(), P(), P(), P()),
        check_vma=False,
    )
```

```python
import functools

import jax
import jax.numpy as jnp
from jax import lax
from jax.experimental import pallas as pl
from jax.experimental.pallas import tpu as pltpu
from jax.sharding import PartitionSpec as P

WIN = 8
PATCH = 4


norm_epsilon = 1e-05


def from_behind(value, axis, steps):
    count = lax.axis_size(axis)
    pairs = [(source, (source + steps) % count) for source in range(count)]
    return lax.ppermute(value, axis, pairs)


def make_patches(pixel_block):
    images, channels, pixel_rows, pixel_cols = pixel_block.shape
    grid_rows = pixel_rows // PATCH
    grid_cols = pixel_cols // PATCH
    shaped = pixel_block.reshape(images, channels, grid_rows, PATCH, grid_cols, PATCH)
    return shaped.transpose(0, 2, 4, 1, 3, 5).reshape(
        images, grid_rows, grid_cols, channels * PATCH * PATCH
    )


def embed_cells(patches, embed_weight, embed_bias):
    return (jnp.dot(patches, embed_weight, preferred_element_type=jnp.float32) + embed_bias).astype(
        jnp.bfloat16
    )


def window_split(block):
    rows_all, cols_all, features = block.shape
    shaped = block.reshape(rows_all // WIN, WIN, cols_all // WIN, WIN, features)
    return shaped.transpose(0, 2, 1, 3, 4).reshape(-1, WIN * WIN, features)


def window_join(windows, rows_all, cols_all):
    features = windows.shape[-1]
    shaped = windows.reshape(rows_all // WIN, cols_all // WIN, WIN, WIN, features)
    return shaped.transpose(0, 2, 1, 3, 4).reshape(rows_all, cols_all, features)

def attend_forward(cell_windows, labels, layer_norm_gain, qkv_full, bias_full):
    window_count, cell_count, features = cell_windows.shape
    head_count = bias_full.shape[0]
    inner_width = qkv_full.shape[1] // 3
    head_size = inner_width // head_count
    score_scale = head_size ** (-0.5)
    flat_rows = cell_windows.reshape(-1, features).astype(jnp.float32)
    average = jnp.mean(flat_rows, axis=-1, keepdims=True)
    centered_input = flat_rows - average
    inverse_deviation = lax.rsqrt(
        jnp.mean(centered_input * centered_input, axis=-1, keepdims=True) + norm_epsilon
    )
    standardized_rows = centered_input * inverse_deviation
    normalized_rows = (standardized_rows * layer_norm_gain).astype(jnp.bfloat16)
    projected = jnp.dot(normalized_rows, qkv_full, preferred_element_type=jnp.float32).astype(
        jnp.bfloat16
    )
    head_shape = (window_count, cell_count, head_count, head_size)
    query_rows = projected[:, :inner_width].reshape(head_shape)
    key_vectors = projected[:, inner_width : 2 * inner_width].reshape(head_shape)
    value_rows = projected[:, 2 * inner_width :].reshape(head_shape)
    scores = (
        jnp.einsum("wmhd,wnhd->whmn", query_rows, key_vectors, preferred_element_type=jnp.float32)
        * score_scale
        + bias_full[None]
    )
    same_region = labels[:, None, :, None] == labels[:, None, None, :]
    scores = jnp.where(same_region, scores, -1e30)
    row_peak = jnp.max(scores, axis=-1, keepdims=True)
    exp_scores = jnp.exp(scores - row_peak)
    attention_weights = exp_scores / jnp.sum(exp_scores, axis=-1, keepdims=True)
    reduced_probability = attention_weights.astype(jnp.bfloat16)
    attended = jnp.einsum(
        "whmn,wnhd->wmhd", reduced_probability, value_rows, preferred_element_type=jnp.float32
    ).astype(jnp.bfloat16)
    stored_residuals = (
        standardized_rows,
        inverse_deviation,
        query_rows,
        key_vectors,
        value_rows,
        attention_weights,
        reduced_probability,
    )
    return (stored_residuals, attended.reshape(-1, inner_width))


def attend_backward(stored_residuals, d_attended, layer_norm_gain, qkv_full):
    (
        standardized_rows,
        inverse_deviation,
        query_rows,
        key_vectors,
        value_rows,
        attention_weights,
        reduced_probability,
    ) = stored_residuals
    head_shape = query_rows.shape
    score_scale = head_shape[3] ** (-0.5)
    total_row_count = standardized_rows.shape[0]
    inner_width = head_shape[2] * head_shape[3]
    d_heads = d_attended.reshape(head_shape)
    d_prob = jnp.einsum("wmhd,wnhd->whmn", d_heads, value_rows, preferred_element_type=jnp.float32)
    d_values = jnp.einsum(
        "whmn,wmhd->wnhd", reduced_probability, d_heads, preferred_element_type=jnp.float32
    ).astype(jnp.bfloat16)
    d_scores = attention_weights * (
        d_prob - jnp.sum(attention_weights * d_prob, axis=-1, keepdims=True)
    )
    table_part = jnp.sum(d_scores, axis=0)
    d_low = d_scores.astype(jnp.bfloat16)
    d_queries = (
        jnp.einsum("whmn,wnhd->wmhd", d_low, key_vectors, preferred_element_type=jnp.float32)
        * score_scale
    ).astype(jnp.bfloat16)
    d_keys = (
        jnp.einsum("whmn,wmhd->wnhd", d_low, query_rows, preferred_element_type=jnp.float32)
        * score_scale
    ).astype(jnp.bfloat16)
    d_projected = jnp.concatenate(
        [
            d_queries.reshape(total_row_count, inner_width),
            d_keys.reshape(total_row_count, inner_width),
            d_values.reshape(total_row_count, inner_width),
        ],
        axis=1,
    )
    normalized_gradient = lax.dot_general(
        d_projected, qkv_full, (((1,), (1,)), ((), ())), preferred_element_type=jnp.float32
    )
    gain_contribution = jnp.sum(normalized_gradient * standardized_rows, axis=0)
    scaled_rows = normalized_gradient * layer_norm_gain
    branch_gradient = inverse_deviation * (
        scaled_rows
        - jnp.mean(scaled_rows, axis=-1, keepdims=True)
        - standardized_rows * jnp.mean(scaled_rows * standardized_rows, axis=-1, keepdims=True)
    )
    return (branch_gradient.astype(jnp.bfloat16), gain_contribution, table_part)


MESH = pl.DeviceIdType.MESH
VMEM = pltpu.VMEM


def greet_everyone(sizes, row, col, dp):
    rows, cols, dps = sizes
    barrier = pltpu.get_barrier_semaphore()
    others = 0
    for r in range(rows):
        for c in range(cols):
            for d in range(dps):
                if r or c or d:
                    others += 1
                    pl.semaphore_signal(
                        barrier,
                        inc=1,
                        device_id={
                            "row": (row + r) % rows,
                            "col": (col + c) % cols,
                            "dp": (dp + d) % dps,
                        },
                        device_id_type=MESH,
                    )
    pl.semaphore_wait(barrier, others)


def gather_kernel(
    sizes, qkv_ref, out_ref, cot_ref, pix_ref,
    qkv_all, out_all, cot_r, cot_c, cot_x, pix_r, pix_c, pix_x,
    send_sem, recv_sem, own_sem, halo_send, halo_recv,
):
    rows, cols, _ = sizes
    ring = rows // 2
    row, col, dp = lax.axis_index("row"), lax.axis_index("col"), lax.axis_index("dp")
    x, z = row % 2, row // 2
    greet_everyone(sizes, row, col, dp)
    gathered = (qkv_all, out_all)
    own = (qkv_ref, out_ref)
    started = []

    def slot(array, ident):
        flag, dy, dx, dz = ident
        column = (col + flag) % 2
        which_row = ((z - dz + ring) % ring) * 2 + (x + dx) % 2
        return gathered[array].at[column * 2 + (dp + dy) % 2, which_row]

    def semaphore(array, ident):
        flag, dy, dx, dz = ident
        return recv_sem.at[array, ((flag * 2 + dy) * 2 + dx) * ring + dz]

    def send(ident, device, landing):
        for array in range(2):
            source = own[array] if ident == (0, 0, 0, 0) else slot(array, ident)
            copy = pltpu.make_async_remote_copy(
                src_ref=source,
                dst_ref=slot(array, ident),
                send_sem=send_sem.at[len(started)],
                recv_sem=semaphore(array, landing),
                device_id=device,
                device_id_type=MESH,
            )
            copy.start()
            started.append(copy)

    def arrive(ident):
        for array in range(2):
            pltpu.make_async_remote_copy(
                src_ref=slot(array, ident),
                dst_ref=slot(array, ident),
                send_sem=send_sem.at[0],
                recv_sem=semaphore(array, ident),
                device_id={"col": (col + 1) % 2},
                device_id_type=MESH,
            ).wait_recv()

    over_y = {"dp": (dp + 1) % 2}
    over_x = {"row": z * 2 + (x + 1) % 2}
    over_core = {"col": (col + 1) % 2}
    along = [s for s in range(1, ring) if s != ring // 2] + [ring // 2]
    for s in along:
        send((0, 0, 0, 0), {"row": ((z + s) % ring) * 2 + x}, (0, 0, 0, s))
    send((0, 0, 0, 0), over_y, (0, 1, 0, 0))
    send((0, 0, 0, 0), over_x, (0, 0, 1, 0))
    send((0, 0, 0, 0), over_core, (1, 0, 0, 0))
    local = [
        pltpu.make_async_copy(own[array], slot(array, (0, 0, 0, 0)), own_sem.at[array])
        for array in range(2)
    ]
    for copy in local:
        copy.start()
    arrive((0, 0, 1, 0))
    send((0, 0, 1, 0), over_y, (0, 1, 1, 0))
    send((0, 0, 1, 0), over_core, (1, 0, 1, 0))
    for s in along:
        arrive((0, 0, 0, s))
        send((0, 0, 0, s), over_x, (0, 0, 1, s))
        send((0, 0, 0, s), over_y, (0, 1, 0, s))
        send((0, 0, 0, s), over_core, (1, 0, 0, s))
    above = (row + rows - 1) % rows
    left = (col + cols - 1) % cols
    edge = cot_c.shape[1]
    halos = []
    for source, target, device in (
        (pix_ref, pix_r, {"row": above}),
        (pix_ref, pix_c, {"col": left}),
        (pix_ref, pix_x, {"row": above, "col": left}),
        (cot_ref, cot_r, {"row": above}),
        (cot_ref.at[:, pl.ds(0, edge)], cot_c, {"col": left}),
        (cot_ref.at[:, pl.ds(0, edge)], cot_x, {"row": above, "col": left}),
    ):
        copy = pltpu.make_async_remote_copy(
            src_ref=source,
            dst_ref=target,
            send_sem=halo_send.at[len(halos)],
            recv_sem=halo_recv.at[len(halos)],
            device_id=device,
            device_id_type=MESH,
        )
        copy.start()
        halos.append(copy)
    for s in along:
        arrive((0, 0, 1, s))
        send((0, 0, 1, s), over_y, (0, 1, 1, s))
        send((0, 0, 1, s), over_core, (1, 0, 1, s))
    for dx, dz in [(0, 0), (1, 0)] + [(0, s) for s in along] + [(1, s) for s in along]:
        arrive((0, 1, dx, dz))
        send((0, 1, dx, dz), over_core, (1, 1, dx, dz))
    for dz in range(ring):
        for dx in range(2):
            for dy in range(2):
                arrive((1, dy, dx, dz))
    for copy in halos:
        copy.wait_recv()
    for copy in started + halos:
        copy.wait_send()
    for copy in local:
        copy.wait()


def gather_inputs(sizes, qkv_weight, out_weight, cot_block, pix_block):
    rows, cols, dps = sizes
    groups = cols * dps
    edge = (cot_block.shape[0], WIN, cot_block.shape[2])
    cot_type, pix_type = cot_block.dtype, pix_block.dtype
    shapes = [
        ((groups, rows) + qkv_weight.shape, qkv_weight.dtype),
        ((groups, rows) + out_weight.shape, out_weight.dtype),
        (cot_block.shape, cot_type),
        (edge, cot_type),
        (edge, cot_type),
        (pix_block.shape, pix_type),
        (pix_block.shape, pix_type),
        (pix_block.shape, pix_type),
    ]
    return pl.pallas_call(
        functools.partial(gather_kernel, sizes),
        out_shape=[jax.ShapeDtypeStruct(shape, kind) for shape, kind in shapes],
        in_specs=[pl.BlockSpec(memory_space=VMEM)] * 4,
        out_specs=[pl.BlockSpec(memory_space=VMEM)] * 8,
        scratch_shapes=[
            pltpu.SemaphoreType.DMA((4 * rows * groups,)),
            pltpu.SemaphoreType.DMA((2, rows * groups)),
            pltpu.SemaphoreType.DMA((2,)),
            pltpu.SemaphoreType.DMA((6,)),
            pltpu.SemaphoreType.DMA((6,)),
        ],
        compiler_params=pltpu.CompilerParams(
            collective_id=0, has_side_effects=True, vmem_limit_bytes=40 * 2**20
        ),
        name="gather_inputs",
    )(qkv_weight, out_weight, cot_block, pix_block)


def reduce_kernel(
    sizes, grad_ref, small_ref, grad_out, small_out,
    core_g, core_e, made_g, made_e, z_g, z_e, acc_g, acc_e,
    xs_g, xs_e, x_g, x_e, ys_g, y_g, ys_e, y_e, tot_e,
    core_send, core_recv, z_send, z_recv, xy_send, xy_recv, all_send, all_recv,
):
    rows, cols, dps = sizes
    ring = rows // 2
    row, col, dp = lax.axis_index("row"), lax.axis_index("col"), lax.axis_index("dp")
    x, z = row % 2, row // 2
    f32, low = jnp.float32, jnp.bfloat16
    greet_everyone(sizes, row, col, dp)
    other = (col + 1) % 2

    def remote(source, target, send_sem, recv_sem, device):
        copy = pltpu.make_async_remote_copy(
            src_ref=source, dst_ref=target, send_sem=send_sem, recv_sem=recv_sem,
            device_id=device, device_id_type=MESH,
        )
        copy.start()
        return copy

    order = [ring // 2] + [s for s in range(1, ring) if s != ring // 2] + [0]
    across = {}
    for s in order:
        there = ((z + s) % ring) * 2
        across[s] = [
            remote(
                source.at[pl.ds(other * 2, 2), pl.ds(there, 2)], target.at[s],
                core_send.at[i, s], core_recv.at[i, s], {"col": other},
            )
            for i, (source, target) in enumerate(((grad_ref, core_g), (small_ref, core_e)))
        ]
    sent = []
    for s in order:
        for copy in across[s]:
            copy.wait_recv()
        there = ((z + s) % ring) * 2
        for d in range(2):
            for h in range(2):
                total = grad_ref[col * 2 + d, there + h].astype(f32) + core_g[s, d, h].astype(f32)
                small = small_ref[col * 2 + d, there + h] + core_e[s, d, h]
                if s:
                    made_g[s, d, h] = total.astype(low)
                    made_e[s, d, h] = small
                else:
                    acc_g[d, h] = total
                    acc_e[d, h] = small
        if s:
            device = {"row": there + x}
            sent.append(remote(made_g.at[s], z_g.at[s], z_send.at[0, s], z_recv.at[0, s], device))
            sent.append(remote(made_e.at[s], z_e.at[s], z_send.at[1, s], z_recv.at[1, s], device))
    for copy in sent:
        copy.wait_recv()

    def z_sum(d, h):
        total, small = acc_g[d, h], acc_e[d, h]
        for s in range(1, ring):
            total = total + z_g[s, d, h].astype(f32)
            small = small + z_e[s, d, h]
        return total, small

    away = (x + 1) % 2
    for d in range(2):
        total, small = z_sum(d, away)
        xs_g[d] = total.astype(low)
        xs_e[d] = small
    device = {"row": z * 2 + away}
    pair = [
        remote(xs_g, x_g, xy_send.at[0], xy_recv.at[0], device),
        remote(xs_e, x_e, xy_send.at[1], xy_recv.at[1], device),
    ]
    mine, mine_small = z_sum(dp, x)
    far, far_small = z_sum((dp + 1) % 2, x)
    for copy in pair:
        copy.wait_recv()
    ys_g[...] = (far + x_g[(dp + 1) % 2].astype(f32)).astype(low)
    ys_e[...] = far_small + x_e[(dp + 1) % 2]
    device = {"dp": (dp + 1) % 2}
    last = [
        remote(ys_e, y_e, xy_send.at[3], xy_recv.at[3], device),
        remote(ys_g, y_g, xy_send.at[2], xy_recv.at[2], device),
    ]
    mine = mine + x_g[dp].astype(f32)
    mine_small = mine_small + x_e[dp]
    last[0].wait_recv()
    group = col * 2 + dp
    whole = mine_small + y_e[...]
    tot_e[...] = whole
    spread = []
    for r in range(rows):
        for c in range(cols):
            for d in range(dps):
                if r or c or d:
                    index = (r * cols + c) * dps + d
                    spread.append(
                        remote(
                            tot_e, small_out.at[group, row],
                            all_send.at[index], all_recv.at[index],
                            {
                                "row": (row + r) % rows,
                                "col": (col + c) % cols,
                                "dp": (dp + d) % dps,
                            },
                        )
                    )
    small_out[group, row] = whole
    last[1].wait_recv()
    grad_out[...] = mine + y_g[...].astype(f32)
    index = 0
    for r in range(rows):
        for c in range(cols):
            for d in range(dps):
                if r or c or d:
                    place = (r * cols + c) * dps + d
                    source_group = ((col + cols - c) % cols) * dps + (dp + dps - d) % dps
                    pltpu.make_async_remote_copy(
                        src_ref=tot_e,
                        dst_ref=small_out.at[source_group, (row + rows - r) % rows],
                        send_sem=all_send.at[place],
                        recv_sem=all_recv.at[place],
                        device_id={"col": other},
                        device_id_type=MESH,
                    ).wait_recv()
    for s in order:
        for copy in across[s]:
            copy.wait_send()
    for copy in sent + pair + last + spread:
        copy.wait_send()


def reduce_outputs(sizes, grad_blocks, small_blocks):
    rows, cols, dps = sizes
    ring = rows // 2
    big, tiny = grad_blocks.shape[2:], small_blocks.shape[2:]
    f32, low = jnp.float32, jnp.bfloat16
    dma = pltpu.SemaphoreType.DMA
    return pl.pallas_call(
        functools.partial(reduce_kernel, sizes),
        out_shape=[
            jax.ShapeDtypeStruct(big, f32),
            jax.ShapeDtypeStruct(small_blocks.shape, f32),
        ],
        in_specs=[pl.BlockSpec(memory_space=VMEM)] * 2,
        out_specs=[pl.BlockSpec(memory_space=VMEM)] * 2,
        scratch_shapes=[
            VMEM((ring, 2, 2) + big, low), VMEM((ring, 2, 2) + tiny, f32),
            VMEM((ring, 2, 2) + big, low), VMEM((ring, 2, 2) + tiny, f32),
            VMEM((ring, 2, 2) + big, low), VMEM((ring, 2, 2) + tiny, f32),
            VMEM((2, 2) + big, f32), VMEM((2, 2) + tiny, f32),
            VMEM((2,) + big, low), VMEM((2,) + tiny, f32),
            VMEM((2,) + big, low), VMEM((2,) + tiny, f32),
            VMEM(big, low), VMEM(big, low), VMEM(tiny, f32), VMEM(tiny, f32), VMEM(tiny, f32),
            dma((2, ring)), dma((2, ring)), dma((2, ring)), dma((2, ring)),
            dma((4,)), dma((4,)),
            dma((rows * cols * dps,)), dma((rows * cols * dps,)),
        ],
        compiler_params=pltpu.CompilerParams(
            collective_id=1, has_side_effects=True, vmem_limit_bytes=40 * 2**20
        ),
        name="reduce_outputs",
    )(grad_blocks, small_blocks)


def block_kernel(
    heads, patch_ref, cot_ref, embed_ref, ebias_ref, gain_ref, qkv_ref, out_ref, bias_ref,
    tag_col_ref, tag_row_ref,
    grad_ref, egrad_ref, bgrad_ref, ggrad_ref, table_ref,
    xhat_ref, proj_ref, datt_ref, att_ref, dproj_ref,
):
    f32, low = jnp.float32, jnp.bfloat16
    groups = qkv_ref.shape[0]
    share, part = qkv_ref.shape[2], out_ref.shape[2]
    inner = out_ref.shape[1]
    size = inner // heads
    cells, features = cot_ref.shape
    repeat = cells // bias_ref.shape[1]
    scale = size ** (-0.5)
    nt = (((1,), (1,)), ((), ()))
    tn = (((0,), (0,)), ((), ()))

    def dot(a, b, dims=(((1,), (0,)), ((), ()))):
        return lax.dot_general(a, b, dims, preferred_element_type=f32)

    gain = gain_ref[...]
    rows = (dot(patch_ref[...], embed_ref[...]) + ebias_ref[...]).astype(low).astype(f32)
    centered = rows - jnp.mean(rows, axis=1, keepdims=True)
    inv_std = lax.rsqrt(jnp.mean(centered * centered, axis=1, keepdims=True) + norm_epsilon)
    xhat_ref[...] = centered * inv_std
    normed = (xhat_ref[...] * gain).astype(low)
    total = None
    for k in range(groups):
        proj_ref[:, k * share : (k + 1) * share] = dot(normed, qkv_ref[k]).astype(low)
        term = dot(cot_ref[:, k * part : (k + 1) * part], out_ref[k], nt)
        total = term if total is None else total + term
    datt_ref[...] = total.astype(low)
    allowed = tag_col_ref[...] == tag_row_ref[...]
    for h in range(heads):
        q = proj_ref[:, h * size : (h + 1) * size]
        key = proj_ref[:, inner + h * size : inner + (h + 1) * size]
        v = proj_ref[:, 2 * inner + h * size : 2 * inner + (h + 1) * size]
        da = datt_ref[:, h * size : (h + 1) * size]
        bias = jnp.concatenate([bias_ref[h]] * repeat, axis=0)
        scores = jnp.where(allowed, dot(q, key, nt) * scale + bias, -1e30)
        weights = jnp.exp(scores - jnp.max(scores, axis=1, keepdims=True))
        prob = weights / jnp.sum(weights, axis=1, keepdims=True)
        prob_low = prob.astype(low)
        att_ref[:, h * size : (h + 1) * size] = dot(prob_low, v).astype(low)
        d_prob = dot(da, v, nt)
        d_scores = prob * (d_prob - jnp.sum(prob * d_prob, axis=1, keepdims=True))
        folded = d_scores[: cells // repeat]
        for w in range(1, repeat):
            folded = folded + d_scores[w * (cells // repeat) : (w + 1) * (cells // repeat)]
        table_ref[h] = folded
        d_low = d_scores.astype(low)
        dproj_ref[:, h * size : (h + 1) * size] = (dot(d_low, key) * scale).astype(low)
        dproj_ref[:, inner + h * size : inner + (h + 1) * size] = (
            dot(d_low, q, tn) * scale
        ).astype(low)
        dproj_ref[:, 2 * inner + h * size : 2 * inner + (h + 1) * size] = dot(
            prob_low, da, tn
        ).astype(low)
    d_normed = None
    for k in range(groups):
        grad_ref[k] = dot(att_ref[...], cot_ref[:, k * part : (k + 1) * part], tn).astype(low)
        term = dot(dproj_ref[:, k * share : (k + 1) * share], qkv_ref[k], nt)
        d_normed = term if d_normed is None else d_normed + term
    xhat = xhat_ref[...]
    ggrad_ref[...] = jnp.sum(d_normed * xhat, axis=0, keepdims=True)
    g = d_normed * gain
    branch = inv_std * (
        g
        - jnp.mean(g, axis=1, keepdims=True)
        - xhat * jnp.mean(g * xhat, axis=1, keepdims=True)
    )
    branch = branch.astype(low)
    patches = patch_ref[...]
    egrad_ref[...] = dot(patches, cot_ref[...], tn) + dot(patches, branch, tn)
    bgrad_ref[...] = jnp.sum(
        cot_ref[...].astype(f32) + branch.astype(f32), axis=0, keepdims=True
    )


def block_grads(patch_rows, cot_rows, embed_weight, embed_bias, gain, qkv_all, out_all, bias_full, labels):
    f32, low = jnp.float32, jnp.bfloat16
    cells, features = cot_rows.shape
    heads, span = bias_full.shape[:2]
    inner = out_all.shape[1]
    windows = cells // span
    tags = (labels + 4 * jnp.arange(windows, dtype=jnp.int32)[:, None]).reshape(-1)
    vmem = pl.BlockSpec(memory_space=VMEM)
    shapes = [
        (out_all.shape, low),
        ((patch_rows.shape[1], features), f32),
        ((1, features), f32),
        ((1, features), f32),
        ((heads, span, cells), f32),
    ]
    grad, egrad, bgrad, ggrad, table = pl.pallas_call(
        functools.partial(block_kernel, heads),
        out_shape=[jax.ShapeDtypeStruct(shape, kind) for shape, kind in shapes],
        in_specs=[vmem] * 10,
        out_specs=[vmem] * 5,
        scratch_shapes=[
            VMEM((cells, features), f32),
            VMEM((cells, 3 * inner), low),
            VMEM((cells, inner), low),
            VMEM((cells, inner), low),
            VMEM((cells, 3 * inner), low),
        ],
        compiler_params=pltpu.CompilerParams(vmem_limit_bytes=48 * 2**20),
        name="block_grads",
    )(
        patch_rows, cot_rows, embed_weight, embed_bias[None], gain[None], qkv_all, out_all,
        jnp.concatenate([bias_full] * windows, axis=2), tags[:, None], tags[None],
    )
    table_part = table.reshape(heads, span, windows, span).sum(axis=2)
    return grad, egrad, bgrad[0], ggrad[0], table_part


def on_device(
    direct,
    sizes,
    pixels,
    cotangent,
    embed_weight,
    embed_bias,
    layer_norm_gain,
    qkv_weight,
    out_weight,
    bias_table,
    rel_index,
    shifts,
):
    images, rows_dev, cols_dev, features = cotangent.shape
    rows, cols, dps = sizes
    head_count, table_size = bias_table.shape
    pix_block, cot_block = pixels[0], cotangent[0]
    row_shift, col_shift = shifts[0, 0], shifts[0, 1]
    if direct:
        qkv_all, out_all, cot_r, cot_c, cot_x, pix_r, pix_c, pix_x = gather_inputs(
            sizes, qkv_weight, out_weight, cot_block, pix_block
        )
        qkv_all = qkv_all.reshape(cols * dps, -1, qkv_weight.shape[1])
        out_all = out_all.reshape(cols * dps, -1, out_weight.shape[1])
    else:
        qkv_full, out_full = [
            lax.all_gather(
                lax.all_gather(w, "row", axis=0, tiled=True), ("col", "dp"), axis=1, tiled=True
            )
            for w in (qkv_weight, out_weight)
        ]
        pix_r, cot_r = from_behind((pix_block, cot_block), "row", -1)
        pix_c, cot_c = from_behind((pix_block, cot_block[:, :WIN]), "col", -1)
        pix_x, cot_x = from_behind((pix_c, cot_c), "row", -1)
    wide_pix = jnp.concatenate(
        [
            jnp.concatenate([pix_block, pix_c[:, :, : WIN * PATCH]], axis=2),
            jnp.concatenate([pix_r, pix_x[:, :, : WIN * PATCH]], axis=2),
        ],
        axis=1,
    )
    wide_cot = jnp.concatenate(
        [
            jnp.concatenate([cot_block, cot_c], axis=1),
            jnp.concatenate([cot_r, cot_x], axis=1),
        ],
        axis=0,
    )
    wide_patches = make_patches(wide_pix[None])[0]
    patches = lax.dynamic_slice(
        wide_patches, (row_shift, col_shift, 0), (rows_dev, cols_dev, wide_patches.shape[2])
    )
    shifted_cot = lax.dynamic_slice(
        wide_cot, (row_shift, col_shift, 0), (rows_dev, cols_dev, features)
    )
    patch_rows = window_split(patches).reshape(-1, patches.shape[2])
    cot_flat = window_split(shifted_cot).reshape(-1, features)
    grid_rows, grid_cols = rows_dev * rows, cols_dev * cols
    row_ids = lax.axis_index("row") * rows_dev + jnp.arange(rows_dev, dtype=jnp.int32)
    col_ids = lax.axis_index("col") * cols_dev + jnp.arange(cols_dev, dtype=jnp.int32)
    row_part = (row_ids >= grid_rows - row_shift).astype(jnp.int32)
    col_part = (col_ids >= grid_cols - col_shift).astype(jnp.int32)
    region = 2 * row_part[:, None] + col_part[None, :]
    labels = window_split(region[:, :, None])[:, :, 0]
    selector = (
        rel_index.reshape(-1)[:, None] == jnp.arange(table_size, dtype=jnp.int32)[None, :]
    ).astype(jnp.float32)
    bias_full = jnp.dot(selector, bias_table.T, precision=lax.Precision.HIGHEST).T.reshape(
        head_count, WIN * WIN, WIN * WIN
    )
    contract = (((0,), (0,)), ((), ()))
    if not direct:
        cells = embed_cells(patch_rows, embed_weight, embed_bias)
        stored_residuals, attended = attend_forward(
            cells.reshape(-1, WIN * WIN, features), labels, layer_norm_gain, qkv_full, bias_full
        )
        d_attended = lax.dot_general(
            cot_flat, out_full, (((1,), (1,)), ((), ())), preferred_element_type=jnp.float32
        ).astype(jnp.bfloat16)
        d_rows, gain_contribution, table_part = attend_backward(
            stored_residuals, d_attended, layer_norm_gain, qkv_full
        )
        table_grad = jnp.dot(
            table_part.reshape(head_count, -1), selector, precision=lax.Precision.HIGHEST
        )
        contract = (((0,), (0,)), ((), ()))
        back_rows = jnp.concatenate([cot_flat, d_rows], axis=0)
        embed_grad = lax.dot_general(
            jnp.concatenate([patch_rows, patch_rows], axis=0),
            back_rows,
            contract,
            preferred_element_type=jnp.float32,
        )
        bias_grad = jnp.sum(back_rows, axis=0, dtype=jnp.float32)
        partial_rows = lax.psum_scatter(
            lax.dot_general(attended, cot_flat, contract, preferred_element_type=jnp.float32),
            "row",
            scatter_dimension=0,
            tiled=True,
        )
        out_weight_grad = lax.psum_scatter(
            partial_rows, ("col", "dp"), scatter_dimension=1, tiled=True
        )
        totals = lax.psum(
            (embed_grad, bias_grad, gain_contribution, table_grad), ("row", "col", "dp")
        )
        return (out_weight_grad,) + totals
    groups = cols * dps
    grad_blocks, embed_grad, bias_grad, gain_contribution, table_part = block_grads(
        patch_rows, cot_flat, embed_weight, embed_bias, layer_norm_gain, qkv_all, out_all,
        bias_full, labels,
    )
    grad_blocks = grad_blocks.reshape((groups, rows) + out_weight.shape)
    table_grad = jnp.dot(
        table_part.reshape(head_count, -1), selector, precision=lax.Precision.HIGHEST
    )
    pieces = (embed_grad, bias_grad, gain_contribution, table_grad)
    flat = jnp.concatenate([piece.reshape(-1) for piece in pieces])
    unit = groups * rows * 2048
    flat = jnp.pad(flat, (0, -flat.shape[0] % unit))
    out_weight_grad, small = reduce_outputs(
        sizes, grad_blocks, flat.reshape(groups, rows, -1, 256)
    )
    small = small.reshape(-1)
    totals, start = [], 0
    for piece in pieces:
        totals.append(small[start : start + piece.size].reshape(piece.shape))
        start += piece.size
    return (out_weight_grad,) + tuple(totals)


def solution(mesh):
    sizes = tuple(mesh.shape[name] for name in ("row", "col", "dp"))
    direct = sizes[1:] == (2, 2) and sizes[0] == 8
    return jax.shard_map(
        functools.partial(on_device, direct, sizes),
        mesh=mesh,
        in_specs=(
            P("dp", None, "row", "col"),
            P("dp", "row", "col", None),
            P(),
            P(),
            P(),
            P("row", ("col", "dp")),
            P("row", ("col", "dp")),
            P(),
            P(),
            P("dp", None),
        ),
        out_specs=(P("row", ("col", "dp")), P(), P(), P(), P()),
        check_vma=False,
    )
```
